32 devices in a mesh: dp: 2 (over x), ep: 16 (over z, y, core).
Axes of the slice: x: 2, y: 2, z: 4, core: 2. Of those that a mesh axis runs over, the one named last changes fastest.
Arguments:
- tok_in: bfloat16 [2048, 2048], P(('dp', 'ep')), parts along dimension 0
- lat_cache: bfloat16 [2048, 64, 512], P(('dp', 'ep')), parts along dimension 0
- rope_cache: bfloat16 [2048, 64, 64], P(('dp', 'ep')), parts along dimension 0
- tok_pos: int32 [2048], P(('dp', 'ep')), parts along dimension 0
- expert_ids: int32 [2048, 6], P(('dp', 'ep')), parts along dimension 0
- attn_gain: bfloat16 [2048], replicated
- w_query: bfloat16 [2048, 3072], replicated
- w_kvdown: bfloat16 [2048, 576], replicated
- w_ukey: bfloat16 [16, 128, 512], replicated
- w_uval: bfloat16 [16, 512, 128], replicated
- w_out: bfloat16 [2048, 2048], replicated
- ffn_gain: bfloat16 [2048], replicated
- w_router: bfloat16 [2048, 64], replicated
- sh_gate: bfloat16 [2048, 2816], replicated
- sh_up: bfloat16 [2048, 2816], replicated
- sh_down: bfloat16 [2816, 2048], replicated
- ex_gate: bfloat16 [64, 2048, 1408], P('ep')
- ex_up: bfloat16 [64, 2048, 1408], P('ep')
- ex_down: bfloat16 [64, 1408, 2048], P('ep')
Outputs:
- output 1: bfloat16 [2048, 2048], P(('dp', 'ep')), parts along dimension 0
- output 2: bfloat16 [2048, 64, 512], P(('dp', 'ep')), parts along dimension 0
- output 3: bfloat16 [2048, 64, 64], P(('dp', 'ep')), parts along dimension 0
There are 2 independent parts. The reference program is written for one: setup_inputs(seed, part) draws one part's arguments, and reference() takes and returns one part's arrays. A program takes and returns all parts, laid end to end along the dimension named above; an argument that names none is the same for every part.
All inputs are finite; a program needn't handle non-finite values.
Results may differ from the reference program's by a relative error of at most 0.013.
Values are sent between devices in bfloat16 or wider.
A program may use at most 1 GiB of HBM per device.

```python
import jax
import jax.numpy as jnp
from jax import lax

D_MODEL = 2048
EXP_FF = 1408
NUM_EXPERTS = 64
TOP_K = 6
SHARED_FF = 2816
NUM_HEADS = 16
NOPE_DIM = 128
ROPE_DIM = 64
V_DIM = 128
KV_RANK = 512
TOKENS_DEV = 64
SEQ_LEN = 64
EP_SIZE = 16

NUM_TOKENS = EP_SIZE * TOKENS_DEV
QK_DIM = NOPE_DIM + ROPE_DIM
ATTN_SCALE = QK_DIM ** -0.5
ROUTE_SCALE = 2.827
ROPE_BASE = 10000.0
NORM_EPS = 1e-6


def unit_norm(values):
    mean_sq = jnp.mean(jnp.square(values), axis=-1, keepdims=True)
    return values * lax.rsqrt(mean_sq + NORM_EPS)


def rms_norm(values, gain_vec):
    return unit_norm(values) * gain_vec.astype(jnp.float32)


def rope_rotate(values, angle_rad):
    half_dim = values.shape[-1] // 2
    x_first = values[..., :half_dim]
    x_second = values[..., half_dim:]
    cos_part = jnp.cos(angle_rad)
    sin_part = jnp.sin(angle_rad)
    return jnp.concatenate([x_first * cos_part - x_second * sin_part, x_second * cos_part + x_first * sin_part], axis=-1)


def draw_routing(key):
    cap_slots = max(2, -(-2 * TOKENS_DEV * TOP_K // NUM_EXPERTS))
    pick_total = TOKENS_DEV * TOP_K
    hot_count = pick_total // (2 * cap_slots)
    rest_picks = pick_total - hot_count * cap_slots
    cold_count = NUM_EXPERTS - hot_count
    rank_ids = jnp.arange(NUM_EXPERTS)
    extra_one = ((rank_ids >= hot_count) & (rank_ids < hot_count + rest_picks % cold_count)).astype(jnp.int32)
    count_per = jnp.where(rank_ids < hot_count, cap_slots, rest_picks // cold_count + extra_one)
    slot_ends = jnp.cumsum(count_per)
    slot_rank = jnp.sum((jnp.arange(pick_total)[:, None] >= slot_ends[None, :]).astype(jnp.int32), axis=1)
    rank_table = slot_rank.reshape(TOP_K, TOKENS_DEV).T
    key_perm, key_rows, key_pos, key_high, key_low = jax.random.split(key, 5)
    expert_perm = jax.random.permutation(key_perm, NUM_EXPERTS)
    row_perms = jax.vmap(lambda sub_key: jax.random.permutation(sub_key, TOKENS_DEV))(jax.random.split(key_rows, EP_SIZE))
    rank_rows = rank_table[row_perms]
    expert_ids = expert_perm[rank_rows].reshape(NUM_TOKENS, TOP_K).astype(jnp.int32)
    pos_draw = jax.random.randint(key_pos, (NUM_TOKENS,), SEQ_LEN // 4, SEQ_LEN)
    high_slot = jax.random.randint(key_high, (), 0, NUM_TOKENS)
    low_slot = (high_slot + jax.random.randint(key_low, (), 1, NUM_TOKENS)) % NUM_TOKENS
    tok_ids = jnp.arange(NUM_TOKENS)
    tok_pos = jnp.where(tok_ids == high_slot, SEQ_LEN - 1, jnp.where(tok_ids == low_slot, SEQ_LEN // 4, pos_draw)).astype(jnp.int32)
    return expert_ids, tok_pos


def setup_inputs(seed: int = 0, part: int = 0) -> dict:
    base_key = jax.random.key(seed)
    part_keys = jax.random.split(jax.random.fold_in(base_key, part), 4)
    weight_keys = jax.random.split(base_key, 16)
    expert_ids, tok_pos = draw_routing(jax.random.fold_in(part_keys[0], 1))

    def gain_draw(key, size, center):
        return (center + 0.2 * jax.random.normal(key, (size,), jnp.float32)).astype(jnp.bfloat16)

    def weight_draw(key, shape, fan_in, factor):
        return (jax.random.normal(key, shape, jnp.float32) * factor * fan_in ** -0.5).astype(jnp.bfloat16)

    tok_in = jax.random.normal(part_keys[1], (NUM_TOKENS, D_MODEL), jnp.float32).astype(jnp.bfloat16)
    lat_cache = (1.3 * jax.random.normal(part_keys[2], (NUM_TOKENS, SEQ_LEN, KV_RANK), jnp.float32)).astype(jnp.bfloat16)
    rope_cache = jax.random.normal(part_keys[3], (NUM_TOKENS, SEQ_LEN, ROPE_DIM), jnp.float32).astype(jnp.bfloat16)
    return {
        'tok_in': tok_in,
        'lat_cache': lat_cache,
        'rope_cache': rope_cache,
        'tok_pos': tok_pos,
        'expert_ids': expert_ids,
        'attn_gain': gain_draw(weight_keys[0], D_MODEL, 1.0),
        'w_query': weight_draw(weight_keys[1], (D_MODEL, NUM_HEADS * QK_DIM), D_MODEL, 1.0),
        'w_kvdown': weight_draw(weight_keys[2], (D_MODEL, KV_RANK + ROPE_DIM), D_MODEL, 1.0),
        'w_ukey': weight_draw(weight_keys[4], (NUM_HEADS, NOPE_DIM, KV_RANK), NOPE_DIM, 1.0),
        'w_uval': weight_draw(weight_keys[5], (NUM_HEADS, KV_RANK, V_DIM), KV_RANK, 1.0),
        'w_out': weight_draw(weight_keys[6], (NUM_HEADS * V_DIM, D_MODEL), NUM_HEADS * V_DIM, 1.0),
        'ffn_gain': gain_draw(weight_keys[7], D_MODEL, 1.0),
        'w_router': weight_draw(weight_keys[8], (D_MODEL, NUM_EXPERTS), D_MODEL, 2.0),
        'sh_gate': weight_draw(weight_keys[9], (D_MODEL, SHARED_FF), D_MODEL, 1.0),
        'sh_up': weight_draw(weight_keys[10], (D_MODEL, SHARED_FF), D_MODEL, 1.0),
        'sh_down': weight_draw(weight_keys[11], (SHARED_FF, D_MODEL), SHARED_FF, 1.0),
        'ex_gate': weight_draw(weight_keys[12], (NUM_EXPERTS, D_MODEL, EXP_FF), D_MODEL, 1.0),
        'ex_up': weight_draw(weight_keys[13], (NUM_EXPERTS, D_MODEL, EXP_FF), D_MODEL, 1.0),
        'ex_down': weight_draw(weight_keys[14], (NUM_EXPERTS, EXP_FF, D_MODEL), EXP_FF, 1.0),
    }


def reference(tok_in, lat_cache, rope_cache, tok_pos, expert_ids, attn_gain, w_query, w_kvdown, w_ukey, w_uval, w_out, ffn_gain, w_router, sh_gate, sh_up, sh_down, ex_gate, ex_up, ex_down):
    x_wide = tok_in.astype(jnp.float32)
    x_norm = rms_norm(x_wide, attn_gain).astype(jnp.bfloat16)
    q_all = jnp.dot(x_norm, w_query, preferred_element_type=jnp.float32).astype(jnp.bfloat16).reshape(NUM_TOKENS, NUM_HEADS, QK_DIM)
    kv_all = jnp.dot(x_norm, w_kvdown, preferred_element_type=jnp.float32)
    inv_freq = ROPE_BASE ** (-(2.0 * jnp.arange(ROPE_DIM // 2)) / ROPE_DIM)
    angle_rad = tok_pos.astype(jnp.float32)[:, None] * inv_freq[None, :]
    lat_new = unit_norm(kv_all[:, :KV_RANK]).astype(jnp.bfloat16)
    rope_new = rope_rotate(kv_all[:, KV_RANK:], angle_rad).astype(jnp.bfloat16)
    q_rope = rope_rotate(q_all[:, :, NOPE_DIM:].astype(jnp.float32), angle_rad[:, None, :]).astype(jnp.bfloat16)
    q_lat = jnp.einsum('bhn,hnc->bhc', q_all[:, :, :NOPE_DIM].astype(jnp.float32), w_ukey.astype(jnp.float32)).astype(jnp.bfloat16)
    seq_ids = jnp.arange(SEQ_LEN)
    at_pos = (seq_ids[None, :] == tok_pos[:, None])[:, :, None]
    lat_out = jnp.where(at_pos, lat_new[:, None, :], lat_cache)
    rope_out = jnp.where(at_pos, rope_new[:, None, :], rope_cache)

    def one_token(item_tuple):
        q_lat_t, q_rope_t, lat_t, rope_t, pos_t = item_tuple
        scores = jnp.dot(q_lat_t, lat_t.T, preferred_element_type=jnp.float32)
        scores = scores + jnp.dot(q_rope_t, rope_t.T, preferred_element_type=jnp.float32)
        scores = scores * ATTN_SCALE
        visible = seq_ids[None, :] <= pos_t
        scores = jnp.where(visible, scores, -jnp.inf)
        prob_mat = jax.nn.softmax(scores, axis=-1).astype(jnp.bfloat16)
        return jnp.dot(prob_mat, lat_t, preferred_element_type=jnp.float32).astype(jnp.bfloat16)

    o_lat = lax.map(one_token, (q_lat, q_rope, lat_out, rope_out, tok_pos))
    o_heads = jnp.einsum('bhc,hcv->bhv', o_lat.astype(jnp.float32), w_uval.astype(jnp.float32)).astype(jnp.bfloat16)
    attn_out = jnp.dot(o_heads.reshape(NUM_TOKENS, NUM_HEADS * V_DIM), w_out, preferred_element_type=jnp.float32)
    resid_bf = (x_wide + attn_out).astype(jnp.bfloat16)
    h_norm = rms_norm(resid_bf.astype(jnp.float32), ffn_gain).astype(jnp.bfloat16)
    gate_prob = jax.nn.sigmoid(jnp.dot(h_norm, w_router, preferred_element_type=jnp.float32))
    chosen = jnp.take_along_axis(gate_prob, expert_ids, axis=1)
    route_w = ROUTE_SCALE * chosen / jnp.sum(chosen, axis=1, keepdims=True)
    sh_act = (jax.nn.silu(jnp.dot(h_norm, sh_gate, preferred_element_type=jnp.float32)) * jnp.dot(h_norm, sh_up, preferred_element_type=jnp.float32)).astype(jnp.bfloat16)
    shared_out = jnp.dot(sh_act, sh_down, preferred_element_type=jnp.float32)
    flat_rows = jnp.repeat(h_norm, TOP_K, axis=0)
    flat_ids = expert_ids.reshape(NUM_TOKENS * TOP_K)

    def one_choice(item_tuple):
        row_vec, expert = item_tuple
        row_mat = row_vec[None, :]
        gate_val = jnp.dot(row_mat, ex_gate[expert], preferred_element_type=jnp.float32)
        up_val = jnp.dot(row_mat, ex_up[expert], preferred_element_type=jnp.float32)
        act_val = (jax.nn.silu(gate_val) * up_val).astype(jnp.bfloat16)
        return jnp.dot(act_val, ex_down[expert], preferred_element_type=jnp.float32).astype(jnp.bfloat16)[0]

    choice_out = lax.map(one_choice, (flat_rows, flat_ids)).reshape(NUM_TOKENS, TOP_K, D_MODEL)
    routed = jnp.sum(route_w[:, :, None] * choice_out.astype(jnp.float32), axis=1)
    out_hidden = (resid_bf.astype(jnp.float32) + shared_out + routed).astype(jnp.bfloat16)
    return (out_hidden, lat_out, rope_out)
```

```python
import jax
import jax.numpy as jnp
from jax import lax
from jax.experimental import pallas as pl
from jax.experimental.pallas import tpu as pltpu
from jax.sharding import PartitionSpec as P

ROUTE_SCALE = 2.827
ROPE_BASE = 10000.0
NORM_EPS = 1e-6


def unit_norm(values):
    mean_sq = jnp.mean(jnp.square(values), axis=-1, keepdims=True)
    return values * lax.rsqrt(mean_sq + NORM_EPS)


def rms_norm(values, gain_vec):
    return unit_norm(values) * gain_vec.astype(jnp.float32)


def rope_rotate(values, angle_rad):
    half_dim = values.shape[-1] // 2
    x_first = values[..., :half_dim]
    x_second = values[..., half_dim:]
    cos_part = jnp.cos(angle_rad)
    sin_part = jnp.sin(angle_rad)
    return jnp.concatenate([x_first * cos_part - x_second * sin_part, x_second * cos_part + x_first * sin_part], axis=-1)


def attention_block(tok_in, lat_cache, rope_cache, tok_pos, attn_gain, w_query, w_kvdown, w_ukey, w_uval, w_out, ffn_gain):
    num_heads, nope_dim, kv_rank = w_ukey.shape
    rope_dim = rope_cache.shape[-1]
    seq_len = lat_cache.shape[1]
    tok_rows = tok_in.shape[0]
    x_wide = tok_in.astype(jnp.float32)
    x_norm = rms_norm(x_wide, attn_gain).astype(jnp.bfloat16)
    q_all = jnp.dot(x_norm, w_query, preferred_element_type=jnp.float32).astype(jnp.bfloat16).reshape(tok_rows, num_heads, nope_dim + rope_dim)
    kv_all = jnp.dot(x_norm, w_kvdown, preferred_element_type=jnp.float32)
    inv_freq = ROPE_BASE ** (-(2.0 * jnp.arange(rope_dim // 2)) / rope_dim)
    angle_rad = tok_pos.astype(jnp.float32)[:, None] * inv_freq[None, :]
    lat_new = unit_norm(kv_all[:, :kv_rank]).astype(jnp.bfloat16)
    rope_new = rope_rotate(kv_all[:, kv_rank:], angle_rad).astype(jnp.bfloat16)
    q_rope = rope_rotate(q_all[:, :, nope_dim:].astype(jnp.float32), angle_rad[:, None, :]).astype(jnp.bfloat16)
    q_lat = jnp.einsum('bhn,hnc->bhc', q_all[:, :, :nope_dim], w_ukey, preferred_element_type=jnp.float32).astype(jnp.bfloat16)
    seq_ids = jnp.arange(seq_len)
    at_pos = (seq_ids[None, :] == tok_pos[:, None])[:, :, None]
    lat_out = jnp.where(at_pos, lat_new[:, None, :], lat_cache)
    rope_out = jnp.where(at_pos, rope_new[:, None, :], rope_cache)
    scores = jnp.einsum('bhc,bsc->bhs', q_lat, lat_out, preferred_element_type=jnp.float32)
    scores = scores + jnp.einsum('bhr,bsr->bhs', q_rope, rope_out, preferred_element_type=jnp.float32)
    scores = scores * (nope_dim + rope_dim) ** -0.5
    visible = (seq_ids[None, :] <= tok_pos[:, None])[:, None, :]
    scores = jnp.where(visible, scores, -jnp.inf)
    prob_mat = jax.nn.softmax(scores, axis=-1).astype(jnp.bfloat16)
    o_lat = jnp.einsum('bhs,bsc->bhc', prob_mat, lat_out, preferred_element_type=jnp.float32).astype(jnp.bfloat16)
    o_heads = jnp.einsum('bhc,hcv->bhv', o_lat, w_uval, preferred_element_type=jnp.float32).astype(jnp.bfloat16)
    attn_out = jnp.dot(o_heads.reshape(tok_rows, -1), w_out, preferred_element_type=jnp.float32)
    resid_bf = (x_wide + attn_out).astype(jnp.bfloat16)
    h_norm = rms_norm(resid_bf.astype(jnp.float32), ffn_gain).astype(jnp.bfloat16)
    return resid_bf, h_norm, lat_out, rope_out


MESH = pl.DeviceIdType.MESH
NE = 4
CAP = 12
SRC = 4
GRP = SRC * CAP
NCH = 8
NA = 4
NB = 4
AHEAD = 2


def moe_kernel(hx_ref, res_ref, rtr_ref, sg_hbm, su_hbm, sd_hbm, eg_hbm, eu_hbm, ed_hbm, out_ref,
               hall, xbuf, act, sact, sout, abuf, bbuf, sbuf, rbuf, fbuf, zbuf, rly, w3,
               a_sem, b_sem, zup_s, zdn_s, z_r, y_s, y_r, c_s, c_r, s_s, s_r, f_s, f_r, l_s, l_r):
    f32, bf16 = jnp.float32, jnp.bfloat16
    dm = res_ref.shape[1]
    rows = res_ref.shape[0]
    ff = act.shape[2]
    cw = dm // NCH
    me = lax.axis_index("ep")
    z, q = me // 4, me % 4
    qy = jnp.where(q >= 2, q - 2, q + 2)
    qc = jnp.where(q % 2 == 1, q - 1, q + 1)
    qd = 3 - q
    peers = (qc, qy, qd)

    def dev(zz, qq):
        return {"ep": zz * 4 + qq}

    def a_src(u):
        if u < 4:
            return (sg_hbm, su_hbm)[u % 2].at[:, pl.ds((u // 2) * ff, ff)]
        return (eg_hbm, eu_hbm)[u % 2].at[(u - 4) // 2]

    def a_copy(u):
        return pltpu.make_async_copy(a_src(u), abuf.at[u % NA], a_sem.at[u % NA])

    def sd_copy(p, hf):
        return pltpu.make_async_copy(sd_hbm.at[:, :, pl.ds((2 * p + hf) * cw, cw)], bbuf.at[p, pl.ds(2 * hf, 2)], b_sem.at[p, hf])

    def b_copy(cc):
        return pltpu.make_async_copy(ed_hbm.at[:, :, pl.ds(cc * cw, cw)], bbuf.at[cc % NB], b_sem.at[cc % NB, 0])

    for u in range(NA):
        a_copy(u).start()
    for p in range(NCH // 2):
        for hf in range(2):
            sd_copy(p, hf).start()

    bar = pltpu.get_barrier_semaphore()
    for s in range(1, 4):
        pl.semaphore_signal(bar, inc=1, device_id=dev((z + s) % 4, q), device_id_type=MESH)
    for qq in peers:
        pl.semaphore_signal(bar, inc=1, device_id=dev(z, qq), device_id_type=MESH)
    pl.semaphore_wait(bar, 6)

    def rcopy(src, dst, ss, rs, d):
        return pltpu.make_async_remote_copy(src_ref=src, dst_ref=dst, send_sem=ss, recv_sem=rs, device_id=d, device_id_type=MESH)

    def up(src, b):
        return rcopy(src, hall.at[q, b], zup_s.at[b], z_r.at[b], dev(z + 1, q))

    def dn(src, b):
        return rcopy(src, hall.at[q, b], zdn_s.at[b], z_r.at[b], dev(z - 1, q))

    def ysend(src, b):
        return rcopy(src, hall.at[q, b], y_s.at[b], y_r.at[b], dev(z, qy))

    def yrecv(b):
        return rcopy(hall.at[qy, b], hall.at[qy, b], y_s.at[b], y_r.at[b], dev(z, qy))

    def csend(src, qq, k, b):
        return rcopy(src, hall.at[qq, b], c_s.at[k, b], c_r.at[k, b], dev(z, qc))

    @pl.when(z < 3)
    def _():
        up(hx_ref, z).start()

    @pl.when(z > 0)
    def _():
        dn(hx_ref, z).start()

    ysend(hx_ref, z).start()
    csend(hx_ref, q, 0, z).start()
    hall[q, z] = hx_ref[...]

    def gather_step(s):
        if s <= 3:
            @pl.when(z - s >= 0)
            def _():
                b = z - s
                up(hall.at[q, b], b).wait_recv()

                @pl.when(z < 3)
                def _():
                    up(hall.at[q, b], b).start()
                ysend(hall.at[q, b], b).start()
                csend(hall.at[q, b], q, 0, b).start()

            @pl.when(z + s <= 3)
            def _():
                b = z + s
                dn(hall.at[q, b], b).wait_recv()

                @pl.when(z > 0)
                def _():
                    dn(hall.at[q, b], b).start()
                ysend(hall.at[q, b], b).start()
                csend(hall.at[q, b], q, 0, b).start()
        t = s - 1
        for sign in ((1, -1) if t else (1,)):
            b = z - sign * t

            @pl.when((b >= 0) & (b <= 3))
            def _():
                yrecv(b).wait_recv()
                csend(hall.at[qy, b], qy, 1, b).start()

    def dot(a, b):
        return jnp.dot(a, b, preferred_element_type=f32)

    def gate_up(x, sg, su, store):
        def tile(off, width):
            g = dot(x(), abuf[sg, :, pl.ds(off, width)])
            u = dot(x(), abuf[su, :, pl.ds(off, width)])
            store(off, width, (g * jax.nn.sigmoid(g) * u).astype(bf16))

        def body(n, carry):
            tile(pl.multiple_of(n * 256, 256), 256)
            return carry
        lax.fori_loop(0, ff // 256, body, 0)
        if ff % 256:
            tile(ff - ff % 256, ff % 256)

    for j in range(2):
        a_copy(2 * j).wait()
        a_copy(2 * j + 1).wait()

        def put(off, width, v, j=j):
            sact[j, :, pl.ds(off, width)] = v
        gate_up(lambda: hx_ref[:, pl.ds(0, dm)], (2 * j) % NA, (2 * j + 1) % NA, put)
        for u in (2 * j + NA, 2 * j + NA + 1):
            a_copy(u).start()
        gather_step(j + 1)
    for p in range(NCH // 2):
        for hf in range(2):
            sd_copy(p, hf).wait()
            sout[2 * p + hf] = dot(sact[0], bbuf[p, 2 * hf]) + dot(sact[1], bbuf[p, 2 * hf + 1])
        b_copy(p).start()
    gather_step(3)

    def spread():
        ee = lax.broadcasted_iota(jnp.int32, (128, SRC * NE * GRP), 0)
        col = lax.broadcasted_iota(jnp.int32, (1, SRC * NE * GRP), 1)
        col48 = lax.rem(col, GRP)
        col_z = lax.div(col48, CAP)
        col_k = (lax.rem(col48, CAP) + 1).astype(f32)
        blk = lax.div(col, NE * GRP)
        owner = jnp.where(blk == 0, q, jnp.where(blk == 1, qc, jnp.where(blk == 2, qy, qd)))
        rep = (ee == SRC * NE * z + NE * owner + lax.div(lax.rem(col, NE * GRP), GRP)).astype(f32).astype(bf16)
        for b in range(SRC):
            hz = hall[q, b, :, pl.ds(0, dm)]
            code = hall[q, b, :, pl.ds(dm, 128)]
            s = jax.nn.sigmoid(dot(hz, rtr_ref[...]))
            chosen = jnp.where(code.astype(f32) > 0.0, s, 0.0)
            w = ROUTE_SCALE * chosen / jnp.sum(chosen, axis=1, keepdims=True)
            hi = w.astype(bf16)
            r1 = w - hi.astype(f32)
            mid = r1.astype(bf16)
            low = (r1 - mid.astype(f32)).astype(bf16)
            ok = (dot(code, rep) == col_k) & (col_z == b)
            for i, part in enumerate((hi, mid, low)):
                w3[i, pl.ds(b * rows, rows)] = jnp.where(ok, dot(part, rep), 0.0).astype(bf16)

    def select(g):
        nr = NE * GRP
        ee = lax.broadcasted_iota(jnp.int32, (nr, 128), 1)
        ri = lax.broadcasted_iota(jnp.int32, (nr, 128), 0)
        lo = (ee - NE * me) * GRP
        sel = ((ri >= lo) & (ri < lo + GRP)).astype(f32).astype(bf16)
        rcol = lax.broadcasted_iota(jnp.int32, (nr, 1), 0)
        r48 = lax.rem(rcol, GRP)
        row_z = lax.div(r48, CAP)
        row_k = (lax.rem(r48, CAP) + 1).astype(f32)
        code = hall[g, :, :, pl.ds(dm, 128)].reshape(SRC * rows, 128)
        ct = lax.dot_general(sel, code, (((1,), (1,)), ((), ())), preferred_element_type=f32)
        tz = lax.div(lax.broadcasted_iota(jnp.int32, (1, SRC * rows), 1), rows)
        pick = jnp.where((ct == row_k) & (row_z == tz), 1.0, 0.0).astype(bf16)

        def body(n, carry):
            off = pl.multiple_of(n * 512, 512)
            hz = hall[g, :, :, pl.ds(off, 512)].reshape(SRC * rows, 512)
            x = dot(pick, hz).astype(bf16)
            for i in range(NE):
                xbuf[i, g, :, pl.ds(off, 512)] = x[i * GRP:(i + 1) * GRP]
            return carry
        lax.fori_loop(0, dm // 512, body, 0)

    spread()
    select(q)
    gather_step(4)
    select(qy)
    for k, qq in ((0, qc), (1, qd)):
        for b in range(SRC):
            rcopy(hall.at[qq, b], hall.at[qq, b], c_s.at[k, b], c_r.at[k, b], dev(z, qc)).wait_recv()
        select(qq)

    for i in range(NE):
        u = 4 + 2 * i
        a_copy(u).wait()
        a_copy(u + 1).wait()

        def put(off, width, v, i=i):
            act[i, :, pl.ds(off, width)] = v
        gate_up(lambda i=i: xbuf[i].reshape(SRC * GRP, dm), u % NA, (u + 1) % NA, put)
        for v in (u + NA, u + NA + 1):
            if v < 4 + 2 * NE:
                a_copy(v).start()

    def s_copy(cc, j):
        return rcopy(sbuf.at[cc, peers[j]], rbuf.at[cc, j], s_s.at[cc, j], s_r.at[cc, j], dev(z, peers[j]))

    def down(cc):
        b_copy(cc).wait()
        for i in range(NE):
            o = dot(act[i], bbuf[cc % NB, i]).astype(bf16)
            for g in range(4):
                sbuf[cc, g, pl.ds(i * GRP, GRP)] = o[g * GRP:(g + 1) * GRP]
        for j in (2, 1, 0):
            s_copy(cc, j).start()
        if cc + NB < NCH:
            b_copy(cc + NB).start()

    edge = (z == 0) | (z == 3)
    z_edge = jnp.where(z <= 1, 0, 3)
    z_mid = jnp.where(z <= 1, 1, 2)
    z_mid2 = 3 - z_mid
    z_edge2 = 3 - z_edge

    def f_copy(cc, dst_z, k, rk):
        return rcopy(fbuf.at[cc, dst_z], zbuf.at[cc, rk], f_s.at[cc, k], f_r.at[cc, rk], dev(dst_z, q))

    def l_copy(cc):
        return rcopy(fbuf.at[cc, z_edge2], rly.at[cc], l_s.at[cc], l_r.at[cc], dev(z_mid, q))

    def combine(cc):
        for j in range(3):
            s_copy(cc, j).wait_recv()
        got = jnp.concatenate([sbuf[cc, q]] + [rbuf[cc, j] for j in range(3)], axis=0)
        acc = dot(w3[0], got) + (dot(w3[1], got) + dot(w3[2], got))
        fbuf[cc] = acc.reshape(SRC, rows, cw)

        @pl.when(edge)
        def _():
            l_copy(cc).start()
            f_copy(cc, z_mid2, 1, 2).start()
            f_copy(cc, z_mid, 0, 0).start()

        @pl.when(jnp.logical_not(edge))
        def _():
            f_copy(cc, z_mid2, 1, 1).start()
            f_copy(cc, z_edge, 0, 0).start()

    def relay(cc):
        @pl.when(jnp.logical_not(edge))
        def _():
            l_copy(cc).wait_recv()
            fbuf[cc, z_edge2] += rly[cc]
            f_copy(cc, z_edge2, 2, 1).start()

    def final(cc):
        @pl.when(edge)
        def _():
            for rk in range(2):
                f_copy(cc, z_mid, 0, rk).wait_recv()
            cols = pl.ds(cc * cw, cw)
            out_ref[:, cols] = (res_ref[:, cols].astype(f32) + sout[cc] + (fbuf[cc, z] + zbuf[cc, 0] + zbuf[cc, 1])).astype(bf16)

        @pl.when(jnp.logical_not(edge))
        def _():
            for rk in range(3):
                f_copy(cc, z_mid, 0, rk).wait_recv()
            cols = pl.ds(cc * cw, cw)
            out_ref[:, cols] = (res_ref[:, cols].astype(f32) + sout[cc] + (fbuf[cc, z] + zbuf[cc, 0] + zbuf[cc, 1] + zbuf[cc, 2])).astype(bf16)

    for cc in range(AHEAD):
        down(cc)
    for cc in range(NCH):
        if cc + AHEAD < NCH:
            down(cc + AHEAD)
        combine(cc)
        if cc:
            relay(cc - 1)
    relay(NCH - 1)
    for cc in range(NCH):
        final(cc)

    @pl.when(z < 3)
    def _():
        up(hx_ref, z).wait_send()

    @pl.when(z > 0)
    def _():
        dn(hx_ref, z).wait_send()

    for s in range(1, 4):
        @pl.when((z - s >= 0) & (z < 3))
        def _():
            up(hall.at[q, z - s], z - s).wait_send()

        @pl.when((z + s <= 3) & (z > 0))
        def _():
            dn(hall.at[q, z + s], z + s).wait_send()
    for b in range(SRC):
        ysend(hall.at[q, b], b).wait_send()
        csend(hall.at[q, b], q, 0, b).wait_send()
        csend(hall.at[qy, b], qy, 1, b).wait_send()
    for cc in range(NCH):
        for j in range(3):
            s_copy(cc, j).wait_send()
        f_copy(cc, z_mid, 0, 0).wait_send()
        f_copy(cc, z_mid, 1, 0).wait_send()

        @pl.when(edge)
        def _():
            l_copy(cc).wait_send()

        @pl.when(jnp.logical_not(edge))
        def _():
            f_copy(cc, z_edge2, 2, 1).wait_send()


def moe_call(hx, resid, router, sh_gate, sh_up, sh_down, ex_gate, ex_up, ex_down):
    rows, dm = resid.shape
    ff = ex_gate.shape[2]
    cw = dm // NCH
    bf16, f32 = jnp.bfloat16, jnp.float32
    vm = pl.BlockSpec(memory_space=pltpu.VMEM)
    hb = pl.BlockSpec(memory_space=pl.ANY)
    sem = pltpu.SemaphoreType.DMA
    nk = NE * GRP
    return pl.pallas_call(
        moe_kernel,
        out_shape=jax.ShapeDtypeStruct((rows, dm), bf16),
        in_specs=[vm] * 3 + [hb] * 6,
        out_specs=vm,
        scratch_shapes=[
            pltpu.VMEM((4, SRC, rows, dm + 128), bf16),
            pltpu.VMEM((NE, 4, GRP, dm), bf16),
            pltpu.VMEM((NE, SRC * GRP, ff), bf16),
            pltpu.VMEM((2, rows, ff), bf16),
            pltpu.VMEM((NCH, rows, cw), f32),
            pltpu.VMEM((NA, dm, ff), bf16),
            pltpu.VMEM((NB, NE, ff, cw), bf16),
            pltpu.VMEM((NCH, 4, nk, cw), bf16),
            pltpu.VMEM((NCH, 3, nk, cw), bf16),
            pltpu.VMEM((NCH, SRC, rows, cw), f32),
            pltpu.VMEM((NCH, 3, rows, cw), f32),
            pltpu.VMEM((NCH, rows, cw), f32),
            pltpu.VMEM((3, SRC * rows, SRC * nk), bf16),
            sem((NA,)), sem((NB, 2)),
            sem((4,)), sem((4,)), sem((4,)),
            sem((4,)), sem((4,)),
            sem((2, 4)), sem((2, 4)),
            sem((NCH, 3)), sem((NCH, 3)),
            sem((NCH, 3)), sem((NCH, 3)),
            sem((NCH,)), sem((NCH,)),
        ],
        compiler_params=pltpu.CompilerParams(collective_id=0, has_side_effects=True, vmem_limit_bytes=66 * 1024 * 1024 - 2 * 1024 * 1024 - 65536),
        name="moe",
    )(hx, resid, router, sh_gate, sh_up, sh_down.reshape(2, ff, dm), ex_gate, ex_up, ex_down)


def solution(mesh):
    row_one = P(('dp', 'ep'))
    row_two = P(('dp', 'ep'), None)
    row_three = P(('dp', 'ep'), None, None)
    rep_one = P(None)
    rep_two = P(None, None)
    rep_three = P(None, None, None)
    exp_spec = P('ep', None, None)

    def local_step(tok_in, lat_cache, rope_cache, tok_pos, expert_ids, attn_gain, w_query, w_kvdown, w_ukey, w_uval, w_out, ffn_gain, w_router, sh_gate, sh_up, sh_down, ex_gate, ex_up, ex_down):
        resid_bf, h_norm, lat_out, rope_out = attention_block(tok_in, lat_cache, rope_cache, tok_pos, attn_gain, w_query, w_kvdown, w_ukey, w_uval, w_out, ffn_gain)
        num_experts = w_router.shape[1]
        pick = (expert_ids[:, :, None] == jnp.arange(num_experts)[None, None, :]).astype(jnp.int32)
        per_tok = jnp.sum(pick, axis=1)
        code = (per_tok * jnp.cumsum(per_tok, axis=0)).astype(jnp.bfloat16)
        hx = jnp.concatenate([h_norm, jnp.pad(code, ((0, 0), (0, 128 - num_experts)))], axis=1)
        router = jnp.pad(w_router, ((0, 0), (0, 128 - num_experts)))
        out_hidden = moe_call(hx, resid_bf, router, sh_gate, sh_up, sh_down, ex_gate, ex_up, ex_down)
        return out_hidden, lat_out, rope_out

    in_specs = (row_two, row_three, row_three, row_one, row_two, rep_one, rep_two, rep_two, rep_three, rep_three, rep_two, rep_one, rep_two, rep_two, rep_two, rep_two, exp_spec, exp_spec, exp_spec)
    out_specs = (row_two, row_three, row_three)
    return jax.shard_map(local_step, mesh=mesh, in_specs=in_specs, out_specs=out_specs, check_vma=False)
```

```python
import jax
import jax.numpy as jnp
import numpy as np
from jax import lax
from jax.experimental import pallas as pl
from jax.experimental.pallas import tpu as pltpu
from jax.sharding import PartitionSpec as P

ROUTE_SCALE = 2.827
ROPE_BASE = 10000.0
NORM_EPS = 1e-6

MESH = pl.DeviceIdType.MESH
NE = 4
CAP = 12
SRC = 4
GRP = SRC * CAP
NCH = 8
CHUNKS = ((0, 1), (1, 1), (2, 2), (4, 2), (6, 2), (8, 2), (10, 2), (12, 2), (14, 1), (15, 1))
NA = 6
NB = 2
WIDE = 512
NP = 4
AHEAD = 2
TG = 16


def attn_kernel(pos_sm, x_ref, posr_ref, ids_ref, freq_ref, ag_ref, fg_ref, lat_hbm, rope_hbm, wq_hbm, wkv_hbm, wuk_hbm, wuv_hbm, wo_hbm,
                hx_ref, res_ref, lato_hbm, ropeo_hbm,
                lat, rope, wq, wkv, wuk, wuv, wo, abuf, latn, ropen, qlat, qrope, olat, ohead, posb, q_sem, m_sem):
    f32, bf16 = jnp.float32, jnp.bfloat16
    rows, dm = x_ref.shape
    heads, nope, rank = wuk.shape
    rd = rope.shape[2]
    seq = lat.shape[1]
    pairs = heads // 2
    pw = 2 * (nope + rd)

    def dot(a, b):
        return jnp.dot(a, b, preferred_element_type=f32)

    def q_copy(i):
        return pltpu.make_async_copy(wq_hbm.at[:, pl.ds(i * pw, pw)], wq.at[i], q_sem.at[i])

    def m_copy(i):
        src, dst = ((wkv_hbm, wkv), (wuk_hbm, wuk), (lat_hbm, lat), (rope_hbm, rope), (wuv_hbm, wuv), (wo_hbm, wo), (lat, lato_hbm), (rope, ropeo_hbm))[i]
        return pltpu.make_async_copy(src, dst, m_sem.at[i])

    m_copy(0).start()
    q_copy(0).start()
    q_copy(1).start()

    x = x_ref[...].astype(f32)
    scale = lax.rsqrt(jnp.mean(jnp.square(x), axis=-1, keepdims=True) + NORM_EPS)
    abuf[...] = (x * scale * ag_ref[...].astype(f32)[None, :]).astype(bf16)

    def dot_nt(a, b):
        return lax.dot_general(a, b, (((1,), (1,)), ((), ())), preferred_element_type=f32)

    def iota(shape, axis):
        return lax.broadcasted_iota(jnp.int32, shape, axis)

    eye = (iota((rows, rows), 0) == iota((rows, rows), 1)).astype(f32).astype(bf16)
    tri = (iota((rows, rows), 0) <= iota((rows, rows), 1)).astype(f32).astype(bf16)
    expert = iota((128, rows), 0)
    per_tok = jnp.zeros((128, rows), f32)
    for k in range(ids_ref.shape[0]):
        per_tok = per_tok + jnp.where(ids_ref[k:k + 1] == expert, 1.0, 0.0)
    code = (per_tok * dot(per_tok.astype(bf16), tri)).astype(bf16)
    hx_ref[:, :128] = dot_nt(eye, code).astype(bf16)
    posb[...] = dot_nt(eye, jnp.broadcast_to(posr_ref[...].astype(f32), (128, rows)).astype(bf16))
    angle = posb[...] * freq_ref[...]
    cos, sin = jnp.cos(angle), jnp.sin(angle)

    m_copy(0).wait()
    m_copy(1).start()
    for i in range(2, pairs):
        q_copy(i).start()
    for i in range(2, 6):
        m_copy(i).start()
    kv = dot_nt(abuf[...], wkv[pl.ds(0, rank)])
    latn[...] = (kv * lax.rsqrt(jnp.mean(jnp.square(kv), axis=-1, keepdims=True) + NORM_EPS)).astype(bf16).astype(f32)
    kr = dot_nt(abuf[...], wkv[pl.ds(rank, rd)])
    swapped = jnp.concatenate([-kr[:, rd // 2:], kr[:, :rd // 2]], axis=1)
    ropen[...] = (kr * cos[:, :rd] + swapped * sin[:, :rd]).astype(bf16).astype(f32)

    lo_half = lax.broadcasted_iota(jnp.int32, (1, 128), 1) < 64
    lo_quarter = lax.broadcasted_iota(jnp.int32, (1, 128), 1) < rd // 2

    def turn(v):
        swapped = jnp.where(lo_quarter, -pltpu.roll(v, 128 - rd // 2, 1), pltpu.roll(v, rd // 2, 1))
        return (v * cos + swapped * sin).astype(bf16)

    m_copy(1).wait()
    for i in range(pairs):
        q_copy(i).wait()
        qp = dot(abuf[...], wq[i]).astype(bf16)
        t1 = qp[:, 128:256].astype(f32)
        t2 = pltpu.roll(qp[:, 256:].astype(f32), 64, 1)
        odd = jnp.where(lo_half, pltpu.roll(t1, 64, 1), t2).astype(bf16)
        qlat[2 * i] = dot(qp[:, :128], wuk[2 * i]).astype(bf16)
        qlat[2 * i + 1] = dot(odd, wuk[2 * i + 1]).astype(bf16)
        qrope[2 * i] = turn(t1)
        qrope[2 * i + 1] = turn(t2)

    m_copy(2).wait()
    m_copy(3).wait()
    it16 = lax.broadcasted_iota(jnp.int32, (16, 1), 0)

    def update(t, carry):
        p = pos_sm[t]
        base = pl.multiple_of((p // 16) * 16, 16)
        hit = it16 == p - base
        lat[t, pl.ds(base, 16)] = jnp.where(hit, latn[pl.ds(t, 1)], lat[t, pl.ds(base, 16)].astype(f32)).astype(bf16)
        rope[t, pl.ds(base, 16)] = jnp.where(hit, ropen[pl.ds(t, 1)], rope[t, pl.ds(base, 16)].astype(f32)).astype(bf16)
        return carry
    lax.fori_loop(0, rows, update, 0, unroll=8)
    nk = TG * seq
    col = lax.broadcasted_iota(jnp.int32, (1, nk), 1)
    tok = lax.broadcasted_iota(jnp.int32, (TG, 1), 0)
    own = (col // seq) == tok
    col_j = col % seq

    for g in range(rows // TG):
        span = pl.ds(g * TG, TG)
        keys = lat[span].reshape(nk, rank)
        rkeys = rope[span].reshape(nk, rd)
        qg = qlat[:, span].reshape(heads * TG, rank)
        qr = qrope[:, span, pl.ds(0, rd)].reshape(heads * TG, rd)
        sc = dot_nt(qg, keys)
        sc = sc + dot_nt(qr, rkeys)
        sc = (sc * (nope + rd) ** -0.5).reshape(heads, TG, nk)
        seen = own & (col_j <= posb[span, pl.ds(0, 1)].astype(jnp.int32))
        sc = jnp.where(seen[None], sc, -jnp.inf)
        e = jnp.exp(sc - jnp.max(sc, axis=-1, keepdims=True))
        prob = (e / jnp.sum(e, axis=-1, keepdims=True)).astype(bf16).reshape(heads * TG, nk)
        olat[:, span] = dot(prob, keys).astype(bf16).reshape(heads, TG, rank)
        if g == 0:
            m_copy(6).start()
            m_copy(7).start()

    m_copy(4).wait()
    for h in range(heads):
        ohead[:, h * nope:(h + 1) * nope] = dot(olat[h], wuv[h]).astype(bf16)
    m_copy(5).wait()

    def out_tile(n, tot):
        cols = pl.ds(pl.multiple_of(n * 512, 512), 512)
        r = (x_ref[:, cols].astype(f32) + dot(ohead[...], wo[:, cols])).astype(bf16)
        res_ref[:, cols] = r
        rw = r.astype(f32)
        return tot + jnp.sum(rw * rw, axis=1, keepdims=True)
    tot = lax.fori_loop(0, dm // 512, out_tile, jnp.zeros((rows, 1), f32))
    scale = lax.rsqrt(tot / dm + NORM_EPS)
    hx_ref[:, 128:] = (res_ref[...].astype(f32) * scale * fg_ref[...].astype(f32)[None, :]).astype(bf16)
    m_copy(6).wait()
    m_copy(7).wait()


def attn_call(tok_in, lat_cache, rope_cache, tok_pos, expert_ids, attn_gain, w_query, w_kvdown, w_ukey, w_uval, w_out, ffn_gain):
    rows, dm = tok_in.shape
    heads, nope, rank = w_ukey.shape
    seq, rd = rope_cache.shape[1:]
    bf16, f32 = jnp.bfloat16, jnp.float32
    freq = ROPE_BASE ** (-(2.0 * np.arange(rd // 2)) / rd)
    freq = np.tile(freq.astype(np.float32), 128 // (rd // 2))[None, :]
    vm = pl.BlockSpec(memory_space=pltpu.VMEM)
    hb = pl.BlockSpec(memory_space=pl.ANY)
    pw = 2 * (nope + rd)
    return pl.pallas_call(
        attn_kernel,
        out_shape=(
            jax.ShapeDtypeStruct((rows, dm + 128), bf16),
            jax.ShapeDtypeStruct((rows, dm), bf16),
            jax.ShapeDtypeStruct(lat_cache.shape, bf16),
            jax.ShapeDtypeStruct(rope_cache.shape, bf16),
        ),
        in_specs=[pl.BlockSpec(memory_space=pltpu.SMEM)] + [vm] * 6 + [hb] * 7,
        out_specs=(vm, vm, hb, hb),
        scratch_shapes=[
            pltpu.VMEM(lat_cache.shape, bf16),
            pltpu.VMEM(rope_cache.shape, bf16),
            pltpu.VMEM((heads // 2, dm, pw), bf16),
            pltpu.VMEM(w_kvdown.shape[::-1], bf16),
            pltpu.VMEM(w_ukey.shape, bf16),
            pltpu.VMEM(w_uval.shape, bf16),
            pltpu.VMEM(w_out.shape, bf16),
            pltpu.VMEM((rows, dm), bf16),
            pltpu.VMEM((rows, rank), f32),
            pltpu.VMEM((rows, rd), f32),
            pltpu.VMEM((heads, rows, rank), bf16),
            pltpu.VMEM((heads, rows, 128), bf16),
            pltpu.VMEM((heads, rows, rank), bf16),
            pltpu.VMEM((rows, heads * nope), bf16),
            pltpu.VMEM((rows, 128), f32),
            pltpu.SemaphoreType.DMA((heads // 2,)),
            pltpu.SemaphoreType.DMA((8,)),
        ],
        compiler_params=pltpu.CompilerParams(vmem_limit_bytes=60 * 1024 * 1024),
        name="attn",
    )(tok_pos, tok_in, tok_pos[None, :], expert_ids.T, jnp.asarray(freq), attn_gain, ffn_gain,
      lat_cache, rope_cache, w_query, w_kvdown.T, w_ukey, w_uval, w_out)


def moe_kernel(hx_ref, res_ref, rtr_ref, sg_hbm, su_hbm, sd_hbm, eg_hbm, eu_hbm, ed_hbm, out_ref,
               hall, xbuf, act, sact, sout, abuf, bbuf, sbuf, rbuf, fbuf, zbuf, rly, w3, pick,
               a_sem, b_sem, zup_s, zdn_s, z_r, y_s, y_r, c_s, c_r, s_s, s_r, f_s, f_r, l_s, l_r):
    f32, bf16 = jnp.float32, jnp.bfloat16
    dm = res_ref.shape[1]
    rows = res_ref.shape[0]
    ff = act.shape[2]
    cw = dm // NCH
    me = lax.axis_index("ep")
    z, q = me // 4, me % 4
    qy = jnp.where(q >= 2, q - 2, q + 2)
    qc = jnp.where(q % 2 == 1, q - 1, q + 1)
    qd = 3 - q
    peers = (qc, qy, qd)

    def dev(zz, qq):
        return {"ep": zz * 4 + qq}

    def a_src(u):
        if u < 4:
            return (sg_hbm, su_hbm)[u % 2].at[:, pl.ds((u // 2) * ff, ff)]
        return (eg_hbm, eu_hbm)[u % 2].at[(u - 4) // 2]

    def a_copy(u):
        return pltpu.make_async_copy(a_src(u), abuf.at[u % NA], a_sem.at[u % NA])

    def sd_copy(p, hf):
        return pltpu.make_async_copy(sd_hbm.at[:, :, pl.ds((2 * p + hf) * cw, cw)], bbuf.at[p % NB, pl.ds(2 * hf, 2)], b_sem.at[p % NB, hf])

    def b_copy(cc):
        return pltpu.make_async_copy(ed_hbm.at[:, :, pl.ds(cc * cw, cw)], bbuf.at[cc % NB], b_sem.at[cc % NB, 0])

    for u in range(2):
        a_copy(u).start()

    bar = pltpu.get_barrier_semaphore()
    for s in range(1, 4):
        pl.semaphore_signal(bar, inc=1, device_id=dev((z + s) % 4, q), device_id_type=MESH)
    for qq in peers:
        pl.semaphore_signal(bar, inc=1, device_id=dev(z, qq), device_id_type=MESH)
    pl.semaphore_wait(bar, 6)

    def rcopy(src, dst, ss, rs, d):
        return pltpu.make_async_remote_copy(src_ref=src, dst_ref=dst, send_sem=ss, recv_sem=rs, device_id=d, device_id_type=MESH)

    cut = [0] + [128 + dm * k // NP for k in range(1, NP + 1)]

    def part(ref, p):
        return ref.at[:, pl.ds(cut[p], cut[p + 1] - cut[p])]

    def blk(qq, b, p):
        return part(hall.at[qq, b], p)

    def up(src, b, p):
        return rcopy(src, blk(q, b, p), zup_s.at[b, p], z_r.at[b, p], dev(z + 1, q))

    def dn(src, b, p):
        return rcopy(src, blk(q, b, p), zdn_s.at[b, p], z_r.at[b, p], dev(z - 1, q))

    def ysend(src, b, p):
        return rcopy(src, blk(q, b, p), y_s.at[b, p], y_r.at[b, p], dev(z, qy))

    def yrecv(b, p):
        return rcopy(blk(qy, b, p), blk(qy, b, p), y_s.at[b, p], y_r.at[b, p], dev(z, qy))

    def csend(src, qq, k, b, p):
        return rcopy(src, blk(qq, b, p), c_s.at[k, b, p], c_r.at[k, b, p], dev(z, qc))

    for p in range(NP):
        mine = part(hx_ref, p)

        @pl.when(z < 3)
        def _():
            up(mine, z, p).start()

        @pl.when(z > 0)
        def _():
            dn(mine, z, p).start()

        ysend(mine, z, p).start()
    for p in range(NP):
        csend(part(hx_ref, p), q, 0, z, p).start()
    for u in range(2, 4):
        a_copy(u).start()
    hall[q, z] = hx_ref[...]

    def gather_step(s, p):
        if s <= 3:
            @pl.when(z - s >= 0)
            def _():
                b = z - s
                src = blk(q, b, p)
                up(src, b, p).wait_recv()

                @pl.when(z < 3)
                def _():
                    up(src, b, p).start()
                ysend(src, b, p).start()
                csend(src, q, 0, b, p).start()

            @pl.when(z + s <= 3)
            def _():
                b = z + s
                src = blk(q, b, p)
                dn(src, b, p).wait_recv()

                @pl.when(z > 0)
                def _():
                    dn(src, b, p).start()
                ysend(src, b, p).start()
                csend(src, q, 0, b, p).start()
        t = s - 1
        for sign in ((1, -1) if t else (1,)):
            b = z - sign * t

            @pl.when((b >= 0) & (b <= 3))
            def _():
                yrecv(b, p).wait_recv()
                csend(blk(qy, b, p), qy, 1, b, p).start()

    def dot(a, b):
        return jnp.dot(a, b, preferred_element_type=f32)

    def gate_up(x, sg, su, store, lo, hi):
        off = lo
        while off < hi:
            width = min(WIDE, hi - off)
            g = dot(x(), abuf[sg, :, pl.ds(off, width)])
            u = dot(x(), abuf[su, :, pl.ds(off, width)])
            store(off, width, (g * jax.nn.sigmoid(g) * u).astype(bf16))
            off += width

    def sh_put(j):
        def put(off, width, v):
            sact[j, :, pl.ds(off, width)] = v
        return put

    def sh_gate_up(j, part):
        cols = (0, ff // 256 // 2 * 256, ff)
        if part == 0:
            a_copy(2 * j).wait()
            a_copy(2 * j + 1).wait()
        gate_up(lambda: hx_ref[:, pl.ds(128, dm)], (2 * j) % NA, (2 * j + 1) % NA, sh_put(j), cols[part], cols[part + 1])

    def sh_down(p):
        for hf in range(2):
            sd_copy(p, hf).wait()
            sout[2 * p + hf] = dot(sact[0], bbuf[p % NB, 2 * hf]) + dot(sact[1], bbuf[p % NB, 2 * hf + 1])
        if p + NB < NCH // 2:
            for hf in range(2):
                sd_copy(p + NB, hf).start()
        else:
            b_copy(p + NB - NCH // 2).start()

    sh_gate_up(0, 0)
    sh_gate_up(0, 1)
    for p in range(NB):
        for hf in range(2):
            sd_copy(p, hf).start()
    gather_step(1, 0)
    gather_step(1, 1)
    sh_gate_up(1, 0)
    gather_step(1, 2)
    sh_gate_up(1, 1)
    gather_step(1, 3)
    sh_down(0)
    gather_step(2, 0)
    sh_down(1)
    for u in range(4, 4 + NA):
        a_copy(u).start()
    gather_step(2, 1)
    sh_down(2)
    gather_step(2, 2)
    sh_down(3)
    gather_step(2, 3)

    def spread():
        ee = lax.broadcasted_iota(jnp.int32, (rtr_ref.shape[0], SRC * NE * GRP), 0)
        col = lax.broadcasted_iota(jnp.int32, (1, SRC * NE * GRP), 1)
        col48 = lax.rem(col, GRP)
        col_z = lax.div(col48, CAP)
        col_k = (lax.rem(col48, CAP) + 1).astype(f32)
        blk = lax.div(col, NE * GRP)
        owner = jnp.where(blk == 0, q, jnp.where(blk == 1, qc, jnp.where(blk == 2, qy, qd)))
        rep = (ee == SRC * NE * z + NE * owner + lax.div(lax.rem(col, NE * GRP), GRP)).astype(f32).astype(bf16)
        for b in range(SRC):
            hz = hall[q, b, :, pl.ds(128, dm)]
            code = hall[q, b, :, pl.ds(0, rtr_ref.shape[0])]
            s = jax.nn.sigmoid(lax.dot_general(hz, rtr_ref[...], (((1,), (1,)), ((), ())), preferred_element_type=f32))
            chosen = jnp.where(code.astype(f32) > 0.0, s, 0.0)
            w = ROUTE_SCALE * chosen / jnp.sum(chosen, axis=1, keepdims=True)
            hi = w.astype(bf16)
            r1 = w - hi.astype(f32)
            mid = r1.astype(bf16)
            low = (r1 - mid.astype(f32)).astype(bf16)
            ok = (dot(code, rep) == col_k) & (col_z == b)
            for i, part in enumerate((hi, mid, low)):
                w3[i, pl.ds(b * rows, rows)] = jnp.where(ok, dot(part, rep), 0.0).astype(bf16)

    def find(g):
        nr = NE * GRP
        ee = lax.broadcasted_iota(jnp.int32, (nr, 128), 1)
        ri = lax.broadcasted_iota(jnp.int32, (nr, 128), 0)
        lo = (ee - NE * me) * GRP
        sel = ((ri >= lo) & (ri < lo + GRP)).astype(f32).astype(bf16)
        rcol = lax.broadcasted_iota(jnp.int32, (nr, 1), 0)
        r48 = lax.rem(rcol, GRP)
        row_z = lax.div(r48, CAP)
        row_k = (lax.rem(r48, CAP) + 1).astype(f32)
        code = hall[g, :, :, pl.ds(0, 128)].reshape(SRC * rows, 128)
        ct = lax.dot_general(sel, code, (((1,), (1,)), ((), ())), preferred_element_type=f32)
        tz = lax.div(lax.broadcasted_iota(jnp.int32, (1, SRC * rows), 1), rows)
        pick[g] = jnp.where((ct == row_k) & (row_z == tz), 1.0, 0.0).astype(bf16)

    def select(g, p):
        wide = dm // NP
        hz = hall[g, :, :, pl.ds(128 + p * wide, wide)].reshape(SRC * rows, wide)
        x = dot(pick[g], hz).astype(bf16)
        for i in range(NE):
            xbuf[i, g, :, pl.ds(p * wide, wide)] = x[i * GRP:(i + 1) * GRP]

    for p in range(NP):
        gather_step(3, p)
        if p == 0:
            find(q)
        select(q, p)
    for p in range(NP):
        gather_step(4, p)
        for k, qq in ((0, qc), (1, qd)):
            for b in range(SRC):
                rcopy(blk(qq, b, p), blk(qq, b, p), c_s.at[k, b, p], c_r.at[k, b, p], dev(z, qc)).wait_recv()
        for qq in peers:
            if p == 0:
                find(qq)
            select(qq, p)

    def expert(i, carry):
        slot = lax.rem(2 * i + 4, NA)
        for w, src in enumerate((eg_hbm, eu_hbm)):
            pltpu.make_async_copy(src.at[i], abuf.at[slot + w], a_sem.at[slot + w]).wait()

        def put(off, width, v):
            act[i, :, pl.ds(off, width)] = v
        gate_up(lambda: xbuf[i].reshape(SRC * GRP, dm), slot, slot + 1, put, 0, ff)

        @pl.when(i + NA // 2 < NE)
        def _():
            for w, src in enumerate((eg_hbm, eu_hbm)):
                pltpu.make_async_copy(src.at[i + NA // 2], abuf.at[slot + w], a_sem.at[slot + w]).start()
        return carry
    lax.fori_loop(0, NE, expert, 0)

    def s_copy(cc, j):
        g0, n = CHUNKS[cc]
        return rcopy(sbuf.at[pl.ds(g0, n), peers[j]], rbuf.at[pl.ds(g0, n), j], s_s.at[cc, j], s_r.at[cc, j], dev(z, peers[j]))

    def down(cc):
        g0, n = CHUNKS[cc]
        w = g0 * 128 // cw
        off = g0 * 128 % cw
        if off == 0:
            b_copy(w).wait()
        for i in range(NE):
            o = dot(act[i], bbuf[w % NB, i, :, pl.ds(off, n * 128)]).astype(bf16)
            for g in range(4):
                for t in range(n):
                    sbuf[g0 + t, g, pl.ds(i * GRP, GRP)] = o[g * GRP:(g + 1) * GRP, t * 128:(t + 1) * 128]
        for j in (2, 1, 0):
            s_copy(cc, j).start()
        if off + n * 128 == cw and w + NB < NCH:
            b_copy(w + NB).start()

    edge = (z == 0) | (z == 3)
    z_edge = jnp.where(z <= 1, 0, 3)
    z_mid = jnp.where(z <= 1, 1, 2)
    z_mid2 = 3 - z_mid
    z_edge2 = 3 - z_edge

    def f_copy(cc, dst_z, k, rk):
        g0, n = CHUNKS[cc]
        return rcopy(fbuf.at[pl.ds(g0, n), dst_z], zbuf.at[pl.ds(g0, n), rk], f_s.at[cc, k], f_r.at[cc, rk], dev(dst_z, q))

    def l_copy(cc):
        g0, n = CHUNKS[cc]
        return rcopy(fbuf.at[pl.ds(g0, n), z_edge2], rly.at[pl.ds(g0, n)], l_s.at[cc], l_r.at[cc], dev(z_mid, q))

    def combine(cc):
        g0, n = CHUNKS[cc]
        for j in range(3):
            s_copy(cc, j).wait_recv()
        got = jnp.concatenate([jnp.concatenate([sbuf[g0 + t, q]] + [rbuf[g0 + t, j] for j in range(3)], axis=0) for t in range(n)], axis=1)
        acc = dot(w3[0], got) + (dot(w3[1], got) + dot(w3[2], got))
        for t in range(n):
            fbuf[g0 + t] = acc[:, t * 128:(t + 1) * 128].reshape(SRC, rows, 128)

        @pl.when(edge)
        def _():
            l_copy(cc).start()
            f_copy(cc, z_mid2, 1, 2).start()
            f_copy(cc, z_mid, 0, 0).start()

        @pl.when(jnp.logical_not(edge))
        def _():
            f_copy(cc, z_mid2, 1, 1).start()
            f_copy(cc, z_edge, 0, 0).start()

    def relay(cc):
        g0, n = CHUNKS[cc]

        @pl.when(jnp.logical_not(edge))
        def _():
            l_copy(cc).wait_recv()
            for t in range(g0, g0 + n):
                fbuf[t, z_edge2] += rly[t]
            f_copy(cc, z_edge2, 2, 1).start()

    def final(cc):
        g0, n = CHUNKS[cc]

        def finish(parts):
            for rk in range(parts):
                f_copy(cc, z_mid, 0, rk).wait_recv()
            for t in range(g0, g0 + n):
                cols = pl.ds(t * 128, 128)
                tot = fbuf[t, z]
                for rk in range(parts):
                    tot = tot + zbuf[t, rk]
                sh = sout[t * 128 // cw, :, pl.ds(t * 128 % cw, 128)]
                out_ref[:, cols] = (res_ref[:, cols].astype(f32) + sh + tot).astype(bf16)

        @pl.when(edge)
        def _():
            finish(2)

        @pl.when(jnp.logical_not(edge))
        def _():
            finish(3)

    last = len(CHUNKS) - 1
    for cc in range(AHEAD):
        down(cc)
    spread()
    for cc in range(last + 1):
        if cc + AHEAD <= last:
            down(cc + AHEAD)
        combine(cc)
        if cc:
            relay(cc - 1)
    relay(last)
    for cc in range(last + 1):
        final(cc)

    for p in range(NP):
        @pl.when(z < 3)
        def _():
            up(part(hx_ref, p), z, p).wait_send()

        @pl.when(z > 0)
        def _():
            dn(part(hx_ref, p), z, p).wait_send()

        for s in range(1, 4):
            @pl.when((z - s >= 0) & (z < 3))
            def _():
                up(blk(q, z - s, p), z - s, p).wait_send()

            @pl.when((z + s <= 3) & (z > 0))
            def _():
                dn(blk(q, z + s, p), z + s, p).wait_send()
        for b in range(SRC):
            ysend(blk(q, b, p), b, p).wait_send()
            csend(blk(q, b, p), q, 0, b, p).wait_send()
            csend(blk(qy, b, p), qy, 1, b, p).wait_send()
    for cc in range(last + 1):
        for j in range(3):
            s_copy(cc, j).wait_send()
        f_copy(cc, z_mid, 0, 0).wait_send()
        f_copy(cc, z_mid, 1, 0).wait_send()

        @pl.when(edge)
        def _():
            l_copy(cc).wait_send()

        @pl.when(jnp.logical_not(edge))
        def _():
            f_copy(cc, z_edge2, 2, 1).wait_send()


def moe_call(hx, resid, router, sh_gate, sh_up, sh_down, ex_gate, ex_up, ex_down):
    rows, dm = resid.shape
    ff = ex_gate.shape[2]
    cw = dm // NCH
    bf16, f32 = jnp.bfloat16, jnp.float32
    vm = pl.BlockSpec(memory_space=pltpu.VMEM)
    hb = pl.BlockSpec(memory_space=pl.ANY)
    sem = pltpu.SemaphoreType.DMA
    nk = NE * GRP
    return pl.pallas_call(
        moe_kernel,
        out_shape=jax.ShapeDtypeStruct((rows, dm), bf16),
        in_specs=[vm] * 3 + [hb] * 6,
        out_specs=vm,
        scratch_shapes=[
            pltpu.VMEM((4, SRC, rows, dm + 128), bf16),
            pltpu.VMEM((NE, 4, GRP, dm), bf16),
            pltpu.VMEM((NE, SRC * GRP, ff), bf16),
            pltpu.VMEM((2, rows, ff), bf16),
            pltpu.VMEM((NCH, rows, cw), f32),
            pltpu.VMEM((NA, dm, ff), bf16),
            pltpu.VMEM((NB, NE, ff, cw), bf16),
            pltpu.VMEM((dm // 128, 4, nk, 128), bf16),
            pltpu.VMEM((dm // 128, 3, nk, 128), bf16),
            pltpu.VMEM((dm // 128, SRC, rows, 128), f32),
            pltpu.VMEM((dm // 128, 3, rows, 128), f32),
            pltpu.VMEM((dm // 128, rows, 128), f32),
            pltpu.VMEM((3, SRC * rows, SRC * nk), bf16),
            pltpu.VMEM((4, nk, SRC * rows), bf16),
            sem((NA,)), sem((NB, 2)),
            sem((4, NP)), sem((4, NP)), sem((4, NP)),
            sem((4, NP)), sem((4, NP)),
            sem((2, 4, NP)), sem((2, 4, NP)),
            sem((len(CHUNKS), 3)), sem((len(CHUNKS), 3)),
            sem((len(CHUNKS), 3)), sem((len(CHUNKS), 3)),
            sem((len(CHUNKS),)), sem((len(CHUNKS),)),
        ],
        compiler_params=pltpu.CompilerParams(collective_id=0, has_side_effects=True, vmem_limit_bytes=66 * 1024 * 1024 - 2 * 1024 * 1024 - 65536),
        name="moe",
    )(hx, resid, router.T, sh_gate, sh_up, sh_down.reshape(2, ff, dm), ex_gate, ex_up, ex_down)


def solution(mesh):
    row_one = P(('dp', 'ep'))
    row_two = P(('dp', 'ep'), None)
    row_three = P(('dp', 'ep'), None, None)
    rep_one = P(None)
    rep_two = P(None, None)
    rep_three = P(None, None, None)
    exp_spec = P('ep', None, None)

    def local_step(tok_in, lat_cache, rope_cache, tok_pos, expert_ids, attn_gain, w_query, w_kvdown, w_ukey, w_uval, w_out, ffn_gain, w_router, sh_gate, sh_up, sh_down, ex_gate, ex_up, ex_down):
        hx, resid, lat_out, rope_out = attn_call(tok_in, lat_cache, rope_cache, tok_pos, expert_ids, attn_gain, w_query, w_kvdown, w_ukey, w_uval, w_out, ffn_gain)
        out_hidden = moe_call(hx, resid, w_router, sh_gate, sh_up, sh_down, ex_gate, ex_up, ex_down)
        return out_hidden, lat_out, rope_out

    in_specs = (row_two, row_three, row_three, row_one, row_two, rep_one, rep_two, rep_two, rep_three, rep_three, rep_two, rep_one, rep_two, rep_two, rep_two, rep_two, exp_spec, exp_spec, exp_spec)
    out_specs = (row_two, row_three, row_three)
    return jax.shard_map(local_step, mesh=mesh, in_specs=in_specs, out_specs=out_specs, check_vma=False)
```

```python
import jax
import jax.numpy as jnp
import numpy as np
from jax import lax
from jax.experimental import pallas as pl
from jax.experimental.pallas import tpu as pltpu
from jax.sharding import PartitionSpec as P

ROUTE_SCALE = 2.827
ROPE_BASE = 10000.0
NORM_EPS = 1e-6

MESH = pl.DeviceIdType.MESH
NE = 4
CAP = 12
SRC = 4
GRP = SRC * CAP
NCH = 8
CHUNKS = ((0, 1), (1, 1), (2, 2), (4, 2), (6, 2), (8, 2), (10, 2), (12, 2), (14, 1), (15, 1))
NA = 6
NB = 2
WIDE = 512
NP = 4
AHEAD = 2
TG = 16


def attn_kernel(pos_sm, x_ref, posr_ref, ids_ref, freq_ref, ag_ref, fg_ref, lat_hbm, rope_hbm, wq_hbm, wkv_hbm, wuk_hbm, wuv_hbm, wo_hbm,
                hx_ref, res_ref, lato_hbm, ropeo_hbm,
                lat, rope, wq, wkv, wuk, wuv, wo, abuf, latn, ropen, qlat, qrope, olat, ohead, posb, q_sem, m_sem):
    f32, bf16 = jnp.float32, jnp.bfloat16
    rows, dm = x_ref.shape
    heads, nope, rank = wuk.shape
    rd = rope.shape[2]
    seq = lat.shape[1]
    pairs = heads // 2
    pw = 2 * (nope + rd)

    def dot(a, b):
        return jnp.dot(a, b, preferred_element_type=f32)

    def q_copy(i):
        return pltpu.make_async_copy(wq_hbm.at[:, pl.ds(i * pw, pw)], wq.at[i], q_sem.at[i])

    def m_copy(i):
        src, dst = ((wkv_hbm, wkv), (wuk_hbm, wuk), (lat_hbm, lat), (rope_hbm, rope), (wuv_hbm, wuv), (wo_hbm, wo), (lat, lato_hbm), (rope, ropeo_hbm))[i]
        return pltpu.make_async_copy(src, dst, m_sem.at[i])

    m_copy(0).start()
    m_copy(1).start()
    q_copy(0).start()
    q_copy(1).start()

    x = x_ref[...].astype(f32)
    scale = lax.rsqrt(jnp.mean(jnp.square(x), axis=-1, keepdims=True) + NORM_EPS)
    abuf[...] = (x * scale * ag_ref[...].astype(f32)[None, :]).astype(bf16)

    def dot_nt(a, b):
        return lax.dot_general(a, b, (((1,), (1,)), ((), ())), preferred_element_type=f32)

    def iota(shape, axis):
        return lax.broadcasted_iota(jnp.int32, shape, axis)

    eye = (iota((rows, rows), 0) == iota((rows, rows), 1)).astype(f32).astype(bf16)
    tri = (iota((rows, rows), 0) <= iota((rows, rows), 1)).astype(f32).astype(bf16)
    expert = iota((128, rows), 0)
    per_tok = jnp.zeros((128, rows), f32)
    for k in range(ids_ref.shape[0]):
        per_tok = per_tok + jnp.where(ids_ref[k:k + 1] == expert, 1.0, 0.0)
    code = (per_tok * dot(per_tok.astype(bf16), tri)).astype(bf16)
    hx_ref[:, :128] = dot_nt(eye, code).astype(bf16)
    posb[...] = dot_nt(eye, jnp.broadcast_to(posr_ref[...].astype(f32), (128, rows)).astype(bf16))
    angle = posb[...] * freq_ref[...]
    cos, sin = jnp.cos(angle), jnp.sin(angle)

    m_copy(0).wait()
    for i in range(2, pairs):
        q_copy(i).start()
    for i in range(2, 6):
        m_copy(i).start()
    kv = dot_nt(abuf[...], wkv[pl.ds(0, rank)])
    latn[...] = (kv * lax.rsqrt(jnp.mean(jnp.square(kv), axis=-1, keepdims=True) + NORM_EPS)).astype(bf16).astype(f32)
    kr = dot_nt(abuf[...], wkv[pl.ds(rank, rd)])
    swapped = jnp.concatenate([-kr[:, rd // 2:], kr[:, :rd // 2]], axis=1)
    ropen[...] = (kr * cos[:, :rd] + swapped * sin[:, :rd]).astype(bf16).astype(f32)

    lo_half = lax.broadcasted_iota(jnp.int32, (1, 128), 1) < 64
    lo_quarter = lax.broadcasted_iota(jnp.int32, (1, 128), 1) < rd // 2

    def turn(v):
        swapped = jnp.where(lo_quarter, -pltpu.roll(v, 128 - rd // 2, 1), pltpu.roll(v, rd // 2, 1))
        return (v * cos + swapped * sin).astype(bf16)

    m_copy(1).wait()
    for i in range(pairs):
        q_copy(i).wait()
        qp = dot(abuf[...], wq[i]).astype(bf16)
        t1 = qp[:, 128:256].astype(f32)
        t2 = pltpu.roll(qp[:, 256:].astype(f32), 64, 1)
        odd = jnp.where(lo_half, pltpu.roll(t1, 64, 1), t2).astype(bf16)
        qlat[2 * i] = dot(qp[:, :128], wuk[2 * i]).astype(bf16)
        qlat[2 * i + 1] = dot(odd, wuk[2 * i + 1]).astype(bf16)
        qrope[2 * i] = turn(t1)
        qrope[2 * i + 1] = turn(t2)

    m_copy(2).wait()
    m_copy(3).wait()
    it16 = lax.broadcasted_iota(jnp.int32, (16, 1), 0)

    def update(t, carry):
        p = pos_sm[t]
        base = pl.multiple_of((p // 16) * 16, 16)
        hit = it16 == p - base
        lat[t, pl.ds(base, 16)] = jnp.where(hit, latn[pl.ds(t, 1)], lat[t, pl.ds(base, 16)].astype(f32)).astype(bf16)
        rope[t, pl.ds(base, 16)] = jnp.where(hit, ropen[pl.ds(t, 1)], rope[t, pl.ds(base, 16)].astype(f32)).astype(bf16)
        return carry
    lax.fori_loop(0, rows, update, 0, unroll=8)
    nk = TG * seq
    col = lax.broadcasted_iota(jnp.int32, (1, nk), 1)
    tok = lax.broadcasted_iota(jnp.int32, (TG, 1), 0)
    own = (col // seq) == tok
    col_j = col % seq

    for g in range(rows // TG):
        span = pl.ds(g * TG, TG)
        keys = lat[span].reshape(nk, rank)
        rkeys = rope[span].reshape(nk, rd)
        qg = qlat[:, span].reshape(heads * TG, rank)
        qr = qrope[:, span, pl.ds(0, rd)].reshape(heads * TG, rd)
        sc = dot_nt(qg, keys)
        sc = sc + dot_nt(qr, rkeys)
        sc = (sc * (nope + rd) ** -0.5).reshape(heads, TG, nk)
        seen = own & (col_j <= posb[span, pl.ds(0, 1)].astype(jnp.int32))
        sc = jnp.where(seen[None], sc, -jnp.inf)
        e = jnp.exp(sc - jnp.max(sc, axis=-1, keepdims=True))
        prob = (e / jnp.sum(e, axis=-1, keepdims=True)).astype(bf16).reshape(heads * TG, nk)
        olat[:, span] = dot(prob, keys).astype(bf16).reshape(heads, TG, rank)
        if g == 0:
            m_copy(6).start()
            m_copy(7).start()

    m_copy(4).wait()
    for h in range(heads):
        ohead[:, h * nope:(h + 1) * nope] = dot(olat[h], wuv[h]).astype(bf16)
    m_copy(5).wait()

    tot = jnp.zeros((rows, 1), f32)
    for n in range(dm // 512):
        cols = pl.ds(n * 512, 512)
        r = (x_ref[:, cols].astype(f32) + dot(ohead[...], wo[:, cols])).astype(bf16)
        res_ref[:, cols] = r
        rw = r.astype(f32)
        tot = tot + jnp.sum(rw * rw, axis=1, keepdims=True)
    scale = lax.rsqrt(tot / dm + NORM_EPS)
    hx_ref[:, 128:] = (res_ref[...].astype(f32) * scale * fg_ref[...].astype(f32)[None, :]).astype(bf16)
    m_copy(6).wait()
    m_copy(7).wait()


def attn_call(tok_in, lat_cache, rope_cache, tok_pos, expert_ids, attn_gain, w_query, w_kvdown, w_ukey, w_uval, w_out, ffn_gain):
    rows, dm = tok_in.shape
    heads, nope, rank = w_ukey.shape
    seq, rd = rope_cache.shape[1:]
    bf16, f32 = jnp.bfloat16, jnp.float32
    freq = ROPE_BASE ** (-(2.0 * np.arange(rd // 2)) / rd)
    freq = np.tile(freq.astype(np.float32), 128 // (rd // 2))[None, :]
    vm = pl.BlockSpec(memory_space=pltpu.VMEM)
    hb = pl.BlockSpec(memory_space=pl.ANY)
    pw = 2 * (nope + rd)
    return pl.pallas_call(
        attn_kernel,
        out_shape=(
            jax.ShapeDtypeStruct((rows, dm + 128), bf16),
            jax.ShapeDtypeStruct((rows, dm), bf16),
            jax.ShapeDtypeStruct(lat_cache.shape, bf16),
            jax.ShapeDtypeStruct(rope_cache.shape, bf16),
        ),
        in_specs=[pl.BlockSpec(memory_space=pltpu.SMEM)] + [vm] * 6 + [hb] * 7,
        out_specs=(vm, vm, hb, hb),
        scratch_shapes=[
            pltpu.VMEM(lat_cache.shape, bf16),
            pltpu.VMEM(rope_cache.shape, bf16),
            pltpu.VMEM((heads // 2, dm, pw), bf16),
            pltpu.VMEM(w_kvdown.shape[::-1], bf16),
            pltpu.VMEM(w_ukey.shape, bf16),
            pltpu.VMEM(w_uval.shape, bf16),
            pltpu.VMEM(w_out.shape, bf16),
            pltpu.VMEM((rows, dm), bf16),
            pltpu.VMEM((rows, rank), f32),
            pltpu.VMEM((rows, rd), f32),
            pltpu.VMEM((heads, rows, rank), bf16),
            pltpu.VMEM((heads, rows, 128), bf16),
            pltpu.VMEM((heads, rows, rank), bf16),
            pltpu.VMEM((rows, heads * nope), bf16),
            pltpu.VMEM((rows, 128), f32),
            pltpu.SemaphoreType.DMA((heads // 2,)),
            pltpu.SemaphoreType.DMA((8,)),
        ],
        compiler_params=pltpu.CompilerParams(vmem_limit_bytes=60 * 1024 * 1024),
        name="attn",
    )(tok_pos, tok_in, tok_pos[None, :], expert_ids.T, jnp.asarray(freq), attn_gain, ffn_gain,
      lat_cache, rope_cache, w_query, w_kvdown.T, w_ukey, w_uval, w_out)


def moe_kernel(hx_ref, res_ref, rtr_ref, sg_hbm, su_hbm, sd_hbm, eg_hbm, eu_hbm, ed_hbm, out_ref,
               hall, xbuf, act, sact, sout, abuf, bbuf, sbuf, rbuf, fbuf, zbuf, rly, w3, pick,
               a_sem, b_sem, zup_s, zdn_s, z_r, y_s, y_r, xu_s, xd_s, x_r, c_s, c_r, s_s, s_r, f_s, f_r, l_s, l_r):
    f32, bf16 = jnp.float32, jnp.bfloat16
    dm = res_ref.shape[1]
    rows = res_ref.shape[0]
    ff = act.shape[2]
    cw = dm // NCH
    me = lax.axis_index("ep")
    z, q = me // 4, me % 4
    qy = jnp.where(q >= 2, q - 2, q + 2)
    qc = jnp.where(q % 2 == 1, q - 1, q + 1)
    qd = 3 - q
    peers = (qc, qy, qd)

    def fenced(f):
        def run(*args):
            @pl.when(me >= 0)
            def _():
                f(*args)
        return run

    def dev(zz, qq):
        return {"ep": zz * 4 + qq}

    def a_src(u):
        if u < 4:
            return (sg_hbm, su_hbm)[u % 2].at[:, pl.ds((u // 2) * ff, ff)]
        return (eg_hbm, eu_hbm)[u % 2].at[(u - 4) // 2]

    def a_copy(u):
        return pltpu.make_async_copy(a_src(u), abuf.at[u % NA], a_sem.at[u % NA])

    def sd_copy(p, hf):
        return pltpu.make_async_copy(sd_hbm.at[:, :, pl.ds((2 * p + hf) * cw, cw)], bbuf.at[p % NB, pl.ds(2 * hf, 2)], b_sem.at[p % NB, hf])

    def b_copy(cc):
        return pltpu.make_async_copy(ed_hbm.at[:, :, pl.ds(cc * cw, cw)], bbuf.at[cc % NB], b_sem.at[cc % NB, 0])

    for u in range(2):
        a_copy(u).start()

    bar = pltpu.get_barrier_semaphore()
    for s in range(1, 4):
        pl.semaphore_signal(bar, inc=1, device_id=dev((z + s) % 4, q), device_id_type=MESH)
    for qq in peers:
        pl.semaphore_signal(bar, inc=1, device_id=dev(z, qq), device_id_type=MESH)
    pl.semaphore_wait(bar, 6)

    def rcopy(src, dst, ss, rs, d):
        return pltpu.make_async_remote_copy(src_ref=src, dst_ref=dst, send_sem=ss, recv_sem=rs, device_id=d, device_id_type=MESH)

    cut = [0] + [128 + dm * k // NP for k in range(1, NP + 1)]

    def part(ref, p):
        return ref.at[:, pl.ds(cut[p], cut[p + 1] - cut[p])]

    def blk(qq, b, p):
        return part(hall.at[qq, b], p)

    def up(src, b, p):
        return rcopy(src, blk(q, b, p), zup_s.at[b, p], z_r.at[b, p], dev(z + 1, q))

    def dn(src, b, p):
        return rcopy(src, blk(q, b, p), zdn_s.at[b, p], z_r.at[b, p], dev(z - 1, q))

    def ysend(src, b, p):
        return rcopy(src, blk(q, b, p), y_s.at[b, p], y_r.at[b, p], dev(z, qy))

    def yrecv(b, p):
        return rcopy(blk(qy, b, p), blk(qy, b, p), y_s.at[b, p], y_r.at[b, p], dev(z, qy))

    def csend(src, qq, k, b, p):
        return rcopy(src, blk(qq, b, p), c_s.at[k, b, p], c_r.at[k, b, p], dev(z, qc))

    for p in range(NP):
        mine = part(hx_ref, p)

        @pl.when(z < 3)
        def _():
            up(mine, z, p).start()

        @pl.when(z > 0)
        def _():
            dn(mine, z, p).start()

        ysend(mine, z, p).start()
    for p in range(NP):
        csend(part(hx_ref, p), q, 0, z, p).start()
    for u in range(2, 4):
        a_copy(u).start()
    hall[q, z] = hx_ref[...]

    def xup(p):
        return rcopy(blk(qy, 0, p), blk(qy, 0, p), xu_s.at[p], x_r.at[0, p], dev(z + 1, q))

    def xdn(p):
        return rcopy(blk(qy, 3, p), blk(qy, 3, p), xd_s.at[p], x_r.at[1, p], dev(z - 1, q))

    @fenced
    def gather_step(s, p):
        late = p >= NP // 2
        if s <= 3:
            @pl.when(z - s >= 0)
            def _():
                b = z - s
                src = blk(q, b, p)
                up(src, b, p).wait_recv()

                @pl.when(z < 3)
                def _():
                    up(src, b, p).start()

                @pl.when((b > 0) | (not late))
                def _():
                    ysend(src, b, p).start()
                csend(src, q, 0, b, p).start()

            @pl.when(z + s <= 3)
            def _():
                b = z + s
                src = blk(q, b, p)
                dn(src, b, p).wait_recv()

                @pl.when(z > 0)
                def _():
                    dn(src, b, p).start()

                @pl.when((b < 3) | (not late))
                def _():
                    ysend(src, b, p).start()
                csend(src, q, 0, b, p).start()
        t = s - 1
        if t == 0:
            yrecv(z, p).wait_recv()
            csend(blk(qy, z, p), qy, 1, z, p).start()
            if late:
                @pl.when(z == 0)
                def _():
                    xup(p).start()

                @pl.when(z == 3)
                def _():
                    xdn(p).start()
            return

        def over_y(b):
            yrecv(b, p).wait_recv()
            csend(blk(qy, b, p), qy, 1, b, p).start()

        @pl.when((z - t > 0) if late else (z - t >= 0))
        def _():
            over_y(z - t)

        @pl.when((z + t < 3) if late else (z + t <= 3))
        def _():
            over_y(z + t)

        if late:
            @pl.when(z == t)
            def _():
                xup(p).wait_recv()

                @pl.when(z < 3)
                def _():
                    xup(p).start()
                csend(blk(qy, 0, p), qy, 1, 0, p).start()

            @pl.when(z == 3 - t)
            def _():
                xdn(p).wait_recv()

                @pl.when(z > 0)
                def _():
                    xdn(p).start()
                csend(blk(qy, 3, p), qy, 1, 3, p).start()

    def dot(a, b):
        return jnp.dot(a, b, preferred_element_type=f32)

    def gate_up(x, sg, su, store, lo, hi):
        off = lo
        while off < hi:
            width = min(WIDE, hi - off)
            g = dot(x(), abuf[sg, :, pl.ds(off, width)])
            u = dot(x(), abuf[su, :, pl.ds(off, width)])
            store(off, width, (g * jax.nn.sigmoid(g) * u).astype(bf16))
            off += width

    def sh_put(j):
        def put(off, width, v):
            sact[j, :, pl.ds(off, width)] = v
        return put

    @fenced
    def sh_gate_up(j, part):
        cols = (0, ff // 256 // 2 * 256, ff)
        if part == 0:
            a_copy(2 * j).wait()
            a_copy(2 * j + 1).wait()
        gate_up(lambda: hx_ref[:, pl.ds(128, dm)], (2 * j) % NA, (2 * j + 1) % NA, sh_put(j), cols[part], cols[part + 1])

    @fenced
    def sh_down(p):
        for hf in range(2):
            sd_copy(p, hf).wait()
            sout[2 * p + hf] = dot(sact[0], bbuf[p % NB, 2 * hf]) + dot(sact[1], bbuf[p % NB, 2 * hf + 1])
        if p + NB < NCH // 2:
            for hf in range(2):
                sd_copy(p + NB, hf).start()
        else:
            b_copy(p + NB - NCH // 2).start()

    sh_gate_up(0, 0)
    sh_gate_up(0, 1)
    for p in range(NB):
        for hf in range(2):
            sd_copy(p, hf).start()
    gather_step(1, 0)
    gather_step(1, 1)
    sh_gate_up(1, 0)
    gather_step(1, 2)
    sh_gate_up(1, 1)
    gather_step(1, 3)
    sh_down(0)
    gather_step(2, 0)
    sh_down(1)
    for u in range(4, 4 + NA):
        a_copy(u).start()
    gather_step(2, 1)
    sh_down(2)
    gather_step(2, 2)
    sh_down(3)
    gather_step(2, 3)

    @fenced
    def spread():
        ee = lax.broadcasted_iota(jnp.int32, (rtr_ref.shape[0], SRC * NE * GRP), 0)
        col = lax.broadcasted_iota(jnp.int32, (1, SRC * NE * GRP), 1)
        col48 = lax.rem(col, GRP)
        col_z = lax.div(col48, CAP)
        col_k = (lax.rem(col48, CAP) + 1).astype(f32)
        blk = lax.div(col, NE * GRP)
        owner = jnp.where(blk == 0, q, jnp.where(blk == 1, qc, jnp.where(blk == 2, qy, qd)))
        rep = (ee == SRC * NE * z + NE * owner + lax.div(lax.rem(col, NE * GRP), GRP)).astype(f32).astype(bf16)
        for b in range(SRC):
            hz = hall[q, b, :, pl.ds(128, dm)]
            code = hall[q, b, :, pl.ds(0, rtr_ref.shape[0])]
            s = jax.nn.sigmoid(lax.dot_general(hz, rtr_ref[...], (((1,), (1,)), ((), ())), preferred_element_type=f32))
            chosen = jnp.where(code.astype(f32) > 0.0, s, 0.0)
            w = ROUTE_SCALE * chosen / jnp.sum(chosen, axis=1, keepdims=True)
            hi = w.astype(bf16)
            r1 = w - hi.astype(f32)
            mid = r1.astype(bf16)
            low = (r1 - mid.astype(f32)).astype(bf16)
            ok = (dot(code, rep) == col_k) & (col_z == b)
            for i, part in enumerate((hi, mid, low)):
                w3[i, pl.ds(b * rows, rows)] = jnp.where(ok, dot(part, rep), 0.0).astype(bf16)

    @fenced
    def find(g):
        nr = NE * GRP
        ee = lax.broadcasted_iota(jnp.int32, (nr, 128), 1)
        ri = lax.broadcasted_iota(jnp.int32, (nr, 128), 0)
        lo = (ee - NE * me) * GRP
        sel = ((ri >= lo) & (ri < lo + GRP)).astype(f32).astype(bf16)
        rcol = lax.broadcasted_iota(jnp.int32, (nr, 1), 0)
        r48 = lax.rem(rcol, GRP)
        row_z = lax.div(r48, CAP)
        row_k = (lax.rem(r48, CAP) + 1).astype(f32)
        code = hall[g, :, :, pl.ds(0, 128)].reshape(SRC * rows, 128)
        ct = lax.dot_general(sel, code, (((1,), (1,)), ((), ())), preferred_element_type=f32)
        tz = lax.div(lax.broadcasted_iota(jnp.int32, (1, SRC * rows), 1), rows)
        pick[g] = jnp.where((ct == row_k) & (row_z == tz), 1.0, 0.0).astype(bf16)

    @fenced
    def select(g, p):
        wide = dm // NP
        hz = hall[g, :, :, pl.ds(128 + p * wide, wide)].reshape(SRC * rows, wide)
        x = dot(pick[g], hz).astype(bf16)
        for i in range(NE):
            xbuf[i, g, :, pl.ds(p * wide, wide)] = x[i * GRP:(i + 1) * GRP]

    for p in range(NP):
        gather_step(3, p)
        if p == 0:
            find(q)
        select(q, p)
    gather_step(4, 0)
    for p in range(NP):
        if p + 1 < NP:
            gather_step(4, p + 1)
        for k, qq in ((0, qc), (1, qd)):
            for b in range(SRC):
                rcopy(blk(qq, b, p), blk(qq, b, p), c_s.at[k, b, p], c_r.at[k, b, p], dev(z, qc)).wait_recv()
        for qq in peers:
            if p == 0:
                find(qq)
            select(qq, p)

    def expert(i, carry):
        slot = lax.rem(2 * i + 4, NA)
        for w, src in enumerate((eg_hbm, eu_hbm)):
            pltpu.make_async_copy(src.at[i], abuf.at[slot + w], a_sem.at[slot + w]).wait()

        def put(off, width, v):
            act[i, :, pl.ds(off, width)] = v
        gate_up(lambda: xbuf[i].reshape(SRC * GRP, dm), slot, slot + 1, put, 0, ff)

        @pl.when(i + NA // 2 < NE)
        def _():
            for w, src in enumerate((eg_hbm, eu_hbm)):
                pltpu.make_async_copy(src.at[i + NA // 2], abuf.at[slot + w], a_sem.at[slot + w]).start()
        return carry
    lax.fori_loop(0, NE, expert, 0)

    def s_copy(cc, j):
        g0, n = CHUNKS[cc]
        return rcopy(sbuf.at[pl.ds(g0, n), peers[j]], rbuf.at[pl.ds(g0, n), j], s_s.at[cc, j], s_r.at[cc, j], dev(z, peers[j]))

    @fenced
    def down(cc):
        g0, n = CHUNKS[cc]
        w = g0 * 128 // cw
        off = g0 * 128 % cw
        if off == 0:
            b_copy(w).wait()
        for i in range(NE):
            o = dot(act[i], bbuf[w % NB, i, :, pl.ds(off, n * 128)]).astype(bf16)
            for g in range(4):
                for t in range(n):
                    sbuf[g0 + t, g, pl.ds(i * GRP, GRP)] = o[g * GRP:(g + 1) * GRP, t * 128:(t + 1) * 128]
        for j in (2, 1, 0):
            s_copy(cc, j).start()
        if off + n * 128 == cw and w + NB < NCH:
            b_copy(w + NB).start()

    last = len(CHUNKS) - 1
    edge = (z == 0) | (z == 3)
    z_edge = jnp.where(z <= 1, 0, 3)
    z_mid = jnp.where(z <= 1, 1, 2)
    z_mid2 = 3 - z_mid
    z_edge2 = 3 - z_edge

    def f_copy(cc, dst_z, k, rk):
        g0, n = CHUNKS[cc]
        return rcopy(fbuf.at[pl.ds(g0, n), dst_z], zbuf.at[pl.ds(g0, n), rk], f_s.at[cc, k], f_r.at[cc, rk], dev(dst_z, q))

    def l_copy(cc):
        g0, n = CHUNKS[cc]
        return rcopy(fbuf.at[pl.ds(g0, n), z_edge2], rly.at[pl.ds(g0, n)], l_s.at[cc], l_r.at[cc], dev(z_mid, q))

    @fenced
    def combine(cc):
        g0, n = CHUNKS[cc]
        for j in range(3):
            s_copy(cc, j).wait_recv()
        got = jnp.concatenate([jnp.concatenate([sbuf[g0 + t, q]] + [rbuf[g0 + t, j] for j in range(3)], axis=0) for t in range(n)], axis=1)
        acc = dot(w3[0], got) + (dot(w3[1], got) + dot(w3[2], got))
        for t in range(n):
            fbuf[g0 + t] = acc[:, t * 128:(t + 1) * 128].reshape(SRC, rows, 128)

        @pl.when(edge)
        def _():
            l_copy(cc).start()
            for c in ((cc - 1, cc) if cc == last else (cc,) if cc < last - 1 else ()):
                f_copy(c, z_mid2, 1, 2).start()
                f_copy(c, z_mid, 0, 0).start()

        @pl.when(jnp.logical_not(edge))
        def _():
            f_copy(cc, z_mid2, 1, 1).start()
            f_copy(cc, z_edge, 0, 0).start()

    @fenced
    def relay(cc):
        g0, n = CHUNKS[cc]

        @pl.when(jnp.logical_not(edge))
        def _():
            l_copy(cc).wait_recv()
            for t in range(g0, g0 + n):
                fbuf[t, z_edge2] += rly[t]
            f_copy(cc, z_edge2, 2, 1).start()

    @fenced
    def final(cc):
        g0, n = CHUNKS[cc]

        def finish(parts):
            for rk in range(parts):
                f_copy(cc, z_mid, 0, rk).wait_recv()
            for t in range(g0, g0 + n):
                cols = pl.ds(t * 128, 128)
                tot = fbuf[t, z]
                for rk in range(parts):
                    tot = tot + zbuf[t, rk]
                sh = sout[t * 128 // cw, :, pl.ds(t * 128 % cw, 128)]
                out_ref[:, cols] = (res_ref[:, cols].astype(f32) + sh + tot).astype(bf16)

        @pl.when(edge)
        def _():
            finish(2)

        @pl.when(jnp.logical_not(edge))
        def _():
            finish(3)

    for cc in range(AHEAD):
        down(cc)
    spread()
    for cc in range(last + 1):
        if cc + AHEAD <= last:
            down(cc + AHEAD)
        combine(cc)
        if cc:
            relay(cc - 1)
    relay(last)
    for cc in range(last + 1):
        final(cc)

    for p in range(NP // 2, NP):
        @pl.when(z < 3)
        def _():
            xup(p).wait_send()

        @pl.when(z > 0)
        def _():
            xdn(p).wait_send()

        @pl.when((z == 0) | (z == 3))
        def _():
            ysend(blk(q, z, p), z, p).wait_send()
    for p in range(NP):
        @pl.when(z < 3)
        def _():
            up(part(hx_ref, p), z, p).wait_send()

        @pl.when(z > 0)
        def _():
            dn(part(hx_ref, p), z, p).wait_send()

        for s in range(1, 4):
            @pl.when((z - s >= 0) & (z < 3))
            def _():
                up(blk(q, z - s, p), z - s, p).wait_send()

            @pl.when((z + s <= 3) & (z > 0))
            def _():
                dn(blk(q, z + s, p), z + s, p).wait_send()
        for b in range(SRC):
            if p < NP // 2 or b in (1, 2):
                ysend(blk(q, b, p), b, p).wait_send()
            csend(blk(q, b, p), q, 0, b, p).wait_send()
            csend(blk(qy, b, p), qy, 1, b, p).wait_send()
    for cc in range(last + 1):
        for j in range(3):
            s_copy(cc, j).wait_send()
        f_copy(cc, z_mid, 0, 0).wait_send()
        f_copy(cc, z_mid, 1, 0).wait_send()

        @pl.when(edge)
        def _():
            l_copy(cc).wait_send()

        @pl.when(jnp.logical_not(edge))
        def _():
            f_copy(cc, z_edge2, 2, 1).wait_send()


def moe_call(hx, resid, router, sh_gate, sh_up, sh_down, ex_gate, ex_up, ex_down):
    rows, dm = resid.shape
    ff = ex_gate.shape[2]
    cw = dm // NCH
    bf16, f32 = jnp.bfloat16, jnp.float32
    vm = pl.BlockSpec(memory_space=pltpu.VMEM)
    hb = pl.BlockSpec(memory_space=pl.ANY)
    sem = pltpu.SemaphoreType.DMA
    nk = NE * GRP
    return pl.pallas_call(
        moe_kernel,
        out_shape=jax.ShapeDtypeStruct((rows, dm), bf16),
        in_specs=[vm] * 3 + [hb] * 6,
        out_specs=vm,
        scratch_shapes=[
            pltpu.VMEM((4, SRC, rows, dm + 128), bf16),
            pltpu.VMEM((NE, 4, GRP, dm), bf16),
            pltpu.VMEM((NE, SRC * GRP, ff), bf16),
            pltpu.VMEM((2, rows, ff), bf16),
            pltpu.VMEM((NCH, rows, cw), f32),
            pltpu.VMEM((NA, dm, ff), bf16),
            pltpu.VMEM((NB, NE, ff, cw), bf16),
            pltpu.VMEM((dm // 128, 4, nk, 128), bf16),
            pltpu.VMEM((dm // 128, 3, nk, 128), bf16),
            pltpu.VMEM((dm // 128, SRC, rows, 128), f32),
            pltpu.VMEM((dm // 128, 3, rows, 128), f32),
            pltpu.VMEM((dm // 128, rows, 128), f32),
            pltpu.VMEM((3, SRC * rows, SRC * nk), bf16),
            pltpu.VMEM((4, nk, SRC * rows), bf16),
            sem((NA,)), sem((NB, 2)),
            sem((4, NP)), sem((4, NP)), sem((4, NP)),
            sem((4, NP)), sem((4, NP)),
            sem((NP,)), sem((NP,)), sem((2, NP)),
            sem((2, 4, NP)), sem((2, 4, NP)),
            sem((len(CHUNKS), 3)), sem((len(CHUNKS), 3)),
            sem((len(CHUNKS), 3)), sem((len(CHUNKS), 3)),
            sem((len(CHUNKS),)), sem((len(CHUNKS),)),
        ],
        compiler_params=pltpu.CompilerParams(collective_id=0, has_side_effects=True, vmem_limit_bytes=66 * 1024 * 1024 - 2 * 1024 * 1024 - 65536),
        name="moe",
    )(hx, resid, router.T, sh_gate, sh_up, sh_down.reshape(2, ff, dm), ex_gate, ex_up, ex_down)


def solution(mesh):
    row_one = P(('dp', 'ep'))
    row_two = P(('dp', 'ep'), None)
    row_three = P(('dp', 'ep'), None, None)
    rep_one = P(None)
    rep_two = P(None, None)
    rep_three = P(None, None, None)
    exp_spec = P('ep', None, None)

    def local_step(tok_in, lat_cache, rope_cache, tok_pos, expert_ids, attn_gain, w_query, w_kvdown, w_ukey, w_uval, w_out, ffn_gain, w_router, sh_gate, sh_up, sh_down, ex_gate, ex_up, ex_down):
        hx, resid, lat_out, rope_out = attn_call(tok_in, lat_cache, rope_cache, tok_pos, expert_ids, attn_gain, w_query, w_kvdown, w_ukey, w_uval, w_out, ffn_gain)
        out_hidden = moe_call(hx, resid, w_router, sh_gate, sh_up, sh_down, ex_gate, ex_up, ex_down)
        return out_hidden, lat_out, rope_out

    in_specs = (row_two, row_three, row_three, row_one, row_two, rep_one, rep_two, rep_two, rep_three, rep_three, rep_two, rep_one, rep_two, rep_two, rep_two, rep_two, exp_spec, exp_spec, exp_spec)
    out_specs = (row_two, row_three, row_three)
    return jax.shard_map(local_step, mesh=mesh, in_specs=in_specs, out_specs=out_specs, check_vma=False)
```

```python
import jax
import jax.numpy as jnp
import numpy as np
from jax import lax
from jax.experimental import pallas as pl
from jax.experimental.pallas import tpu as pltpu
from jax.sharding import PartitionSpec as P

ROUTE_SCALE = 2.827
ROPE_BASE = 10000.0
NORM_EPS = 1e-6

MESH = pl.DeviceIdType.MESH
LANE = 128
NE = 4
CAP = 12
SRC = 4
GRP = SRC * CAP
NCH = 8
CHUNKS = ((0, 1), (1, 1), (2, 2), (4, 2), (6, 2), (8, 2), (10, 2), (12, 2), (14, 1), (15, 1))
NA = 6
NB = 2
WIDE = 512
NP = 4
DIRECT = (8, 9)
SETTLED = 4
AHEAD = 2
TG = 16


def attn_kernel(pos_sm, x_ref, posr_ref, ids_ref, freq_ref, ag_ref, fg_ref, lat_hbm, rope_hbm, wq_hbm, wkv_hbm, wuk_hbm, wuv_hbm, wo_hbm,
                hx_ref, res_ref, lato_hbm, ropeo_hbm,
                lat, rope, wq, wkv, wuk, wuv, wo, abuf, latn, ropen, qlat, qrope, olat, ohead, posb, q_sem, m_sem):
    f32, bf16 = jnp.float32, jnp.bfloat16
    rows, dm = x_ref.shape
    heads, nope, rank = wuk.shape
    rd = rope.shape[2]
    seq = lat.shape[1]
    pairs = heads // 2
    pw = 2 * (nope + rd)

    def dot(a, b):
        return jnp.dot(a, b, preferred_element_type=f32)

    def q_copy(i):
        return pltpu.make_async_copy(wq_hbm.at[:, pl.ds(i * pw, pw)], wq.at[i], q_sem.at[i])

    def m_copy(i):
        src, dst = ((wkv_hbm, wkv), (wuk_hbm, wuk), (lat_hbm, lat), (rope_hbm, rope), (wuv_hbm, wuv), (wo_hbm, wo), (lat, lato_hbm), (rope, ropeo_hbm))[i]
        return pltpu.make_async_copy(src, dst, m_sem.at[i])

    m_copy(0).start()
    m_copy(1).start()
    q_copy(0).start()
    q_copy(1).start()

    x = x_ref[...].astype(f32)
    scale = lax.rsqrt(jnp.mean(jnp.square(x), axis=-1, keepdims=True) + NORM_EPS)
    abuf[...] = (x * scale * ag_ref[...].astype(f32)[None, :]).astype(bf16)

    def dot_nt(a, b):
        return lax.dot_general(a, b, (((1,), (1,)), ((), ())), preferred_element_type=f32)

    def iota(shape, axis):
        return lax.broadcasted_iota(jnp.int32, shape, axis)

    eye = (iota((rows, rows), 0) == iota((rows, rows), 1)).astype(f32).astype(bf16)
    tri = (iota((rows, rows), 0) <= iota((rows, rows), 1)).astype(f32).astype(bf16)
    expert = iota((LANE, rows), 0)
    per_tok = jnp.zeros((LANE, rows), f32)
    for k in range(ids_ref.shape[0]):
        per_tok = per_tok + jnp.where(ids_ref[k:k + 1] == expert, 1.0, 0.0)
    code = (per_tok * dot(per_tok.astype(bf16), tri)).astype(bf16)
    hx_ref[:, :LANE] = dot_nt(eye, code).astype(bf16)
    posb[...] = dot_nt(eye, jnp.broadcast_to(posr_ref[...].astype(f32), (LANE, rows)).astype(bf16))
    angle = posb[...] * freq_ref[...]
    cos, sin = jnp.cos(angle), jnp.sin(angle)

    m_copy(0).wait()
    for i in range(2, pairs):
        q_copy(i).start()
    for i in range(2, 6):
        m_copy(i).start()
    kv = dot_nt(abuf[...], wkv[pl.ds(0, rank)])
    latn[...] = (kv * lax.rsqrt(jnp.mean(jnp.square(kv), axis=-1, keepdims=True) + NORM_EPS)).astype(bf16).astype(f32)
    kr = dot_nt(abuf[...], wkv[pl.ds(rank, rd)])
    swapped = jnp.concatenate([-kr[:, rd // 2:], kr[:, :rd // 2]], axis=1)
    ropen[...] = (kr * cos[:, :rd] + swapped * sin[:, :rd]).astype(bf16).astype(f32)

    lo_half = lax.broadcasted_iota(jnp.int32, (1, LANE), 1) < 64
    lo_quarter = lax.broadcasted_iota(jnp.int32, (1, LANE), 1) < rd // 2

    def turn(v):
        swapped = jnp.where(lo_quarter, -pltpu.roll(v, LANE - rd // 2, 1), pltpu.roll(v, rd // 2, 1))
        return (v * cos + swapped * sin).astype(bf16)

    m_copy(1).wait()
    for i in range(pairs):
        q_copy(i).wait()
        qp = dot(abuf[...], wq[i]).astype(bf16)
        t1 = qp[:, LANE:256].astype(f32)
        t2 = pltpu.roll(qp[:, 256:].astype(f32), 64, 1)
        odd = jnp.where(lo_half, pltpu.roll(t1, 64, 1), t2).astype(bf16)
        qlat[2 * i] = dot(qp[:, :LANE], wuk[2 * i]).astype(bf16)
        qlat[2 * i + 1] = dot(odd, wuk[2 * i + 1]).astype(bf16)
        qrope[2 * i] = turn(t1)
        qrope[2 * i + 1] = turn(t2)

    m_copy(2).wait()
    m_copy(3).wait()
    it16 = lax.broadcasted_iota(jnp.int32, (16, 1), 0)

    def update(t, carry):
        p = pos_sm[t]
        base = pl.multiple_of((p // 16) * 16, 16)
        hit = it16 == p - base
        lat[t, pl.ds(base, 16)] = jnp.where(hit, latn[pl.ds(t, 1)], lat[t, pl.ds(base, 16)].astype(f32)).astype(bf16)
        rope[t, pl.ds(base, 16)] = jnp.where(hit, ropen[pl.ds(t, 1)], rope[t, pl.ds(base, 16)].astype(f32)).astype(bf16)
        return carry
    lax.fori_loop(0, rows, update, 0, unroll=8)
    nk = TG * seq
    col = lax.broadcasted_iota(jnp.int32, (1, nk), 1)
    tok = lax.broadcasted_iota(jnp.int32, (TG, 1), 0)
    own = (col // seq) == tok
    col_j = col % seq

    for g in range(rows // TG):
        span = pl.ds(g * TG, TG)
        keys = lat[span].reshape(nk, rank)
        rkeys = rope[span].reshape(nk, rd)
        qg = qlat[:, span].reshape(heads * TG, rank)
        qr = qrope[:, span, pl.ds(0, rd)].reshape(heads * TG, rd)
        sc = dot_nt(qg, keys)
        sc = sc + dot_nt(qr, rkeys)
        sc = (sc * (nope + rd) ** -0.5).reshape(heads, TG, nk)
        seen = own & (col_j <= posb[span, pl.ds(0, 1)].astype(jnp.int32))
        sc = jnp.where(seen[None], sc, -jnp.inf)
        e = jnp.exp(sc - jnp.max(sc, axis=-1, keepdims=True))
        prob = (e / jnp.sum(e, axis=-1, keepdims=True)).astype(bf16).reshape(heads * TG, nk)
        olat[:, span] = dot(prob, keys).astype(bf16).reshape(heads, TG, rank)
        if g == 0:
            m_copy(6).start()
            m_copy(7).start()

    m_copy(4).wait()
    for h in range(heads):
        ohead[:, h * nope:(h + 1) * nope] = dot(olat[h], wuv[h]).astype(bf16)
    m_copy(5).wait()

    tot = jnp.zeros((rows, 1), f32)
    for n in range(dm // 512):
        cols = pl.ds(n * 512, 512)
        r = (x_ref[:, cols].astype(f32) + dot(ohead[...], wo[:, cols])).astype(bf16)
        res_ref[:, cols] = r
        rw = r.astype(f32)
        tot = tot + jnp.sum(rw * rw, axis=1, keepdims=True)
    scale = lax.rsqrt(tot / dm + NORM_EPS)
    hx_ref[:, LANE:] = (res_ref[...].astype(f32) * scale * fg_ref[...].astype(f32)[None, :]).astype(bf16)
    m_copy(6).wait()
    m_copy(7).wait()


def attn_call(tok_in, lat_cache, rope_cache, tok_pos, expert_ids, attn_gain, w_query, w_kvdown, w_ukey, w_uval, w_out, ffn_gain):
    rows, dm = tok_in.shape
    heads, nope, rank = w_ukey.shape
    seq, rd = rope_cache.shape[1:]
    bf16, f32 = jnp.bfloat16, jnp.float32
    freq = ROPE_BASE ** (-(2.0 * np.arange(rd // 2)) / rd)
    freq = np.tile(freq.astype(np.float32), LANE // (rd // 2))[None, :]
    vm = pl.BlockSpec(memory_space=pltpu.VMEM)
    hb = pl.BlockSpec(memory_space=pl.ANY)
    pw = 2 * (nope + rd)
    return pl.pallas_call(
        attn_kernel,
        out_shape=(
            jax.ShapeDtypeStruct((rows, dm + LANE), bf16),
            jax.ShapeDtypeStruct((rows, dm), bf16),
            jax.ShapeDtypeStruct(lat_cache.shape, bf16),
            jax.ShapeDtypeStruct(rope_cache.shape, bf16),
        ),
        in_specs=[pl.BlockSpec(memory_space=pltpu.SMEM)] + [vm] * 6 + [hb] * 7,
        out_specs=(vm, vm, hb, hb),
        scratch_shapes=[
            pltpu.VMEM(lat_cache.shape, bf16),
            pltpu.VMEM(rope_cache.shape, bf16),
            pltpu.VMEM((heads // 2, dm, pw), bf16),
            pltpu.VMEM(w_kvdown.shape[::-1], bf16),
            pltpu.VMEM(w_ukey.shape, bf16),
            pltpu.VMEM(w_uval.shape, bf16),
            pltpu.VMEM(w_out.shape, bf16),
            pltpu.VMEM((rows, dm), bf16),
            pltpu.VMEM((rows, rank), f32),
            pltpu.VMEM((rows, rd), f32),
            pltpu.VMEM((heads, rows, rank), bf16),
            pltpu.VMEM((heads, rows, LANE), bf16),
            pltpu.VMEM((heads, rows, rank), bf16),
            pltpu.VMEM((rows, heads * nope), bf16),
            pltpu.VMEM((rows, LANE), f32),
            pltpu.SemaphoreType.DMA((heads // 2,)),
            pltpu.SemaphoreType.DMA((8,)),
        ],
        compiler_params=pltpu.CompilerParams(vmem_limit_bytes=60 * 1024 * 1024),
        name="attn",
    )(tok_pos, tok_in, tok_pos[None, :], expert_ids.T, jnp.asarray(freq), attn_gain, ffn_gain,
      lat_cache, rope_cache, w_query, w_kvdown.T, w_ukey, w_uval, w_out)


def moe_kernel(hx_ref, res_ref, rtr_ref, sg_hbm, su_hbm, sd_hbm, eg_hbm, eu_hbm, ed_hbm, out_ref,
               hall, xbuf, act, sact, sout, abuf, bbuf, sbuf, rbuf, fbuf, zbuf, rly, w3, pick,
               a_sem, b_sem, zup_s, zdn_s, z_r, y_s, y_r, xu_s, xd_s, x_r, c_s, c_r, s_s, s_r, f_s, f_r, l_s, l_r):
    f32, bf16 = jnp.float32, jnp.bfloat16
    dm = res_ref.shape[1]
    rows = res_ref.shape[0]
    ff = act.shape[2]
    cw = dm // NCH
    me = lax.axis_index("ep")
    z, q = me // 4, me % 4
    qy = jnp.where(q >= 2, q - 2, q + 2)
    qc = jnp.where(q % 2 == 1, q - 1, q + 1)
    qd = 3 - q
    peers = (qc, qy, qd)

    def fenced(f):
        def run(*args):
            @pl.when(me >= 0)
            def _():
                f(*args)
        return run

    def dev(zz, qq):
        return {"ep": zz * 4 + qq}

    def a_src(u):
        if u < 4:
            return (sg_hbm, su_hbm)[u % 2].at[:, pl.ds((u // 2) * ff, ff)]
        return (eg_hbm, eu_hbm)[u % 2].at[(u - 4) // 2]

    def a_copy(u):
        return pltpu.make_async_copy(a_src(u), abuf.at[u % NA], a_sem.at[u % NA])

    def sd_copy(p, hf):
        return pltpu.make_async_copy(sd_hbm.at[:, :, pl.ds((2 * p + hf) * cw, cw)], bbuf.at[p % NB, pl.ds(2 * hf, 2)], b_sem.at[p % NB, hf])

    def b_copy(cc):
        return pltpu.make_async_copy(ed_hbm.at[:, :, pl.ds(cc * cw, cw)], bbuf.at[cc % NB], b_sem.at[cc % NB, 0])

    for u in range(2):
        a_copy(u).start()

    bar = pltpu.get_barrier_semaphore()
    for s in range(1, 4):
        pl.semaphore_signal(bar, inc=1, device_id=dev((z + s) % 4, q), device_id_type=MESH)
    for qq in peers:
        pl.semaphore_signal(bar, inc=1, device_id=dev(z, qq), device_id_type=MESH)
    pl.semaphore_wait(bar, 6)

    def rcopy(src, dst, ss, rs, d):
        return pltpu.make_async_remote_copy(src_ref=src, dst_ref=dst, send_sem=ss, recv_sem=rs, device_id=d, device_id_type=MESH)

    cut = [0] + [LANE + dm * k // NP for k in range(1, NP + 1)]

    def part(ref, p):
        return ref.at[:, pl.ds(cut[p], cut[p + 1] - cut[p])]

    def blk(qq, b, p):
        return part(hall.at[qq, b], p)

    def up(src, b, p):
        return rcopy(src, blk(q, b, p), zup_s.at[b], z_r.at[b, p], dev(z + 1, q))

    def dn(src, b, p):
        return rcopy(src, blk(q, b, p), zdn_s.at[b], z_r.at[b, p], dev(z - 1, q))

    def ysend(src, b, p):
        return rcopy(src, blk(q, b, p), y_s.at[b, p], y_r.at[b, p], dev(z, qy))

    def yrecv(b, p):
        return rcopy(blk(qy, b, p), blk(qy, b, p), y_s.at[b, p], y_r.at[b, p], dev(z, qy))

    def csend(src, qq, k, b, p):
        return rcopy(src, blk(qq, b, p), c_s.at[k, b], c_r.at[k, p], dev(z, qc))

    for p in range(NP):
        mine = part(hx_ref, p)

        @pl.when(z < 3)
        def _():
            up(mine, z, p).start()

        @pl.when(z > 0)
        def _():
            dn(mine, z, p).start()

        ysend(mine, z, p).start()
    for p in range(NP):
        csend(part(hx_ref, p), q, 0, z, p).start()
    for u in range(2, 4):
        a_copy(u).start()
    hall[q, z] = hx_ref[...]

    def xup(p):
        return rcopy(blk(qy, 0, p), blk(qy, 0, p), xu_s.at[p], x_r.at[0, p], dev(z + 1, q))

    def xdn(p):
        return rcopy(blk(qy, 3, p), blk(qy, 3, p), xd_s.at[p], x_r.at[1, p], dev(z - 1, q))

    @fenced
    def gather_step(s, p):
        late = p >= NP // 2
        if s <= 3:
            @pl.when(z - s >= 0)
            def _():
                b = z - s
                src = blk(q, b, p)
                up(src, b, p).wait_recv()

                @pl.when(z < 3)
                def _():
                    up(src, b, p).start()

                @pl.when((b > 0) | (not late))
                def _():
                    ysend(src, b, p).start()
                csend(src, q, 0, b, p).start()

            @pl.when(z + s <= 3)
            def _():
                b = z + s
                src = blk(q, b, p)
                dn(src, b, p).wait_recv()

                @pl.when(z > 0)
                def _():
                    dn(src, b, p).start()

                @pl.when((b < 3) | (not late))
                def _():
                    ysend(src, b, p).start()
                csend(src, q, 0, b, p).start()
        t = s - 1
        if t == 0:
            yrecv(z, p).wait_recv()
            csend(blk(qy, z, p), qy, 1, z, p).start()
            if late:
                @pl.when(z == 0)
                def _():
                    xup(p).start()

                @pl.when(z == 3)
                def _():
                    xdn(p).start()
            return

        def over_y(b):
            yrecv(b, p).wait_recv()
            csend(blk(qy, b, p), qy, 1, b, p).start()

        @pl.when((z - t > 0) if late else (z - t >= 0))
        def _():
            over_y(z - t)

        @pl.when((z + t < 3) if late else (z + t <= 3))
        def _():
            over_y(z + t)

        if late:
            @pl.when(z == t)
            def _():
                xup(p).wait_recv()

                @pl.when(z < 3)
                def _():
                    xup(p).start()
                csend(blk(qy, 0, p), qy, 1, 0, p).start()

            @pl.when(z == 3 - t)
            def _():
                xdn(p).wait_recv()

                @pl.when(z > 0)
                def _():
                    xdn(p).start()
                csend(blk(qy, 3, p), qy, 1, 3, p).start()

    def dot(a, b):
        return jnp.dot(a, b, preferred_element_type=f32)

    def gate_up(x, sg, su, store, lo, hi):
        off = lo
        while off < hi:
            width = min(WIDE, hi - off)
            g = dot(x(), abuf[sg, :, pl.ds(off, width)])
            u = dot(x(), abuf[su, :, pl.ds(off, width)])
            store(off, width, (g * jax.nn.sigmoid(g) * u).astype(bf16))
            off += width

    def sh_put(j):
        def put(off, width, v):
            sact[j, :, pl.ds(off, width)] = v
        return put

    @fenced
    def sh_gate_up(j, part):
        cols = (0, ff // 256 // 2 * 256, ff)
        if part == 0:
            a_copy(2 * j).wait()
            a_copy(2 * j + 1).wait()
        gate_up(lambda: hx_ref[:, pl.ds(LANE, dm)], (2 * j) % NA, (2 * j + 1) % NA, sh_put(j), cols[part], cols[part + 1])

    @fenced
    def sh_down(p):
        for hf in range(2):
            sd_copy(p, hf).wait()
            sout[2 * p + hf] = dot(sact[0], bbuf[p % NB, 2 * hf]) + dot(sact[1], bbuf[p % NB, 2 * hf + 1])
        if p + NB < NCH // 2:
            for hf in range(2):
                sd_copy(p + NB, hf).start()
        else:
            b_copy(p + NB - NCH // 2).start()

    sh_gate_up(0, 0)
    sh_gate_up(0, 1)
    for p in range(NB):
        for hf in range(2):
            sd_copy(p, hf).start()
    gather_step(1, 0)
    gather_step(1, 1)
    sh_gate_up(1, 0)
    gather_step(1, 2)
    sh_gate_up(1, 1)
    gather_step(1, 3)
    sh_down(0)
    gather_step(2, 0)
    sh_down(1)
    for u in range(4, 4 + NA):
        a_copy(u).start()
    gather_step(2, 1)
    sh_down(2)
    gather_step(2, 2)
    sh_down(3)
    gather_step(2, 3)

    @fenced
    def spread():
        ee = lax.broadcasted_iota(jnp.int32, (rtr_ref.shape[0], SRC * NE * GRP), 0)
        col = lax.broadcasted_iota(jnp.int32, (1, SRC * NE * GRP), 1)
        col48 = lax.rem(col, GRP)
        col_z = lax.div(col48, CAP)
        col_k = (lax.rem(col48, CAP) + 1).astype(f32)
        blk = lax.div(col, NE * GRP)
        owner = jnp.where(blk == 0, q, jnp.where(blk == 1, qc, jnp.where(blk == 2, qy, qd)))
        rep = (ee == SRC * NE * z + NE * owner + lax.div(lax.rem(col, NE * GRP), GRP)).astype(f32).astype(bf16)
        for b in range(SRC):
            hz = hall[q, b, :, pl.ds(LANE, dm)]
            code = hall[q, b, :, pl.ds(0, rtr_ref.shape[0])]
            s = jax.nn.sigmoid(lax.dot_general(hz, rtr_ref[...], (((1,), (1,)), ((), ())), preferred_element_type=f32))
            chosen = jnp.where(code.astype(f32) > 0.0, s, 0.0)
            w = ROUTE_SCALE * chosen / jnp.sum(chosen, axis=1, keepdims=True)
            hi = w.astype(bf16)
            r1 = w - hi.astype(f32)
            mid = r1.astype(bf16)
            low = (r1 - mid.astype(f32)).astype(bf16)
            ok = (dot(code, rep) == col_k) & (col_z == b)
            for i, part in enumerate((hi, mid, low)):
                w3[i, pl.ds(b * rows, rows)] = jnp.where(ok, dot(part, rep), 0.0).astype(bf16)

    @fenced
    def find(g):
        nr = NE * GRP
        ee = lax.broadcasted_iota(jnp.int32, (nr, LANE), 1)
        ri = lax.broadcasted_iota(jnp.int32, (nr, LANE), 0)
        lo = (ee - NE * me) * GRP
        sel = ((ri >= lo) & (ri < lo + GRP)).astype(f32).astype(bf16)
        rcol = lax.broadcasted_iota(jnp.int32, (nr, 1), 0)
        r48 = lax.rem(rcol, GRP)
        row_z = lax.div(r48, CAP)
        row_k = (lax.rem(r48, CAP) + 1).astype(f32)
        code = hall[g, :, :, pl.ds(0, LANE)].reshape(SRC * rows, LANE)
        ct = lax.dot_general(sel, code, (((1,), (1,)), ((), ())), preferred_element_type=f32)
        tz = lax.div(lax.broadcasted_iota(jnp.int32, (1, SRC * rows), 1), rows)
        pick[g] = jnp.where((ct == row_k) & (row_z == tz), 1.0, 0.0).astype(bf16)

    @fenced
    def select(g, p):
        wide = dm // NP
        hz = hall[g, :, :, pl.ds(LANE + p * wide, wide)].reshape(SRC * rows, wide)
        x = dot(pick[g], hz).astype(bf16)
        for i in range(NE):
            xbuf[i, g, :, pl.ds(p * wide, wide)] = x[i * GRP:(i + 1) * GRP]

    for p in range(NP):
        gather_step(3, p)
        if p == 0:
            find(q)
        select(q, p)
    gather_step(4, 0)
    for p in range(NP):
        if p + 1 < NP:
            gather_step(4, p + 1)
        for k, qq in ((0, qc), (1, qd)):
            got = hall.at[qq, :, :, pl.ds(cut[p], cut[p + 1] - cut[p])]
            rcopy(got, got, c_s.at[k, 0], c_r.at[k, p], dev(z, qc)).wait_recv()
        for qq in peers:
            if p == 0:
                find(qq)
            select(qq, p)

    def expert(i, carry):
        slot = lax.rem(2 * i + 4, NA)
        for w, src in enumerate((eg_hbm, eu_hbm)):
            pltpu.make_async_copy(src.at[i], abuf.at[slot + w], a_sem.at[slot + w]).wait()

        def put(off, width, v):
            act[i, :, pl.ds(off, width)] = v
        gate_up(lambda: xbuf[i].reshape(SRC * GRP, dm), slot, slot + 1, put, 0, ff)

        @pl.when(i + NA // 2 < NE)
        def _():
            for w, src in enumerate((eg_hbm, eu_hbm)):
                pltpu.make_async_copy(src.at[i + NA // 2], abuf.at[slot + w], a_sem.at[slot + w]).start()
        return carry
    lax.fori_loop(0, NE, expert, 0)

    def s_copy(cc, j):
        g0, n = CHUNKS[cc]
        return rcopy(sbuf.at[pl.ds(g0, n), peers[j]], rbuf.at[pl.ds(g0, n), j], s_s.at[cc, j], s_r.at[cc], dev(z, peers[j]))

    @fenced
    def down(cc):
        g0, n = CHUNKS[cc]
        w = g0 * LANE // cw
        off = g0 * LANE % cw
        if off == 0:
            b_copy(w).wait()
        for i in range(NE):
            o = dot(act[i], bbuf[w % NB, i, :, pl.ds(off, n * LANE)]).astype(bf16)
            for g in range(4):
                for t in range(n):
                    sbuf[g0 + t, g, pl.ds(i * GRP, GRP)] = o[g * GRP:(g + 1) * GRP, t * LANE:(t + 1) * LANE]
        for j in (2, 1, 0):
            s_copy(cc, j).start()
        if off + n * LANE == cw and w + NB < NCH:
            b_copy(w + NB).start()

    last = len(CHUNKS) - 1
    edge = (z == 0) | (z == 3)
    z_edge = jnp.where(z <= 1, 0, 3)
    z_mid = jnp.where(z <= 1, 1, 2)
    z_mid2 = 3 - z_mid
    z_edge2 = 3 - z_edge

    def f_copy(cc, dst_z, k, rk):
        g0, n = CHUNKS[cc]
        return rcopy(fbuf.at[pl.ds(g0, n), dst_z], zbuf.at[pl.ds(g0, n), rk], f_s.at[cc, k], f_r.at[cc], dev(dst_z, q))

    def l_copy(cc):
        g0, n = CHUNKS[cc]
        return rcopy(fbuf.at[pl.ds(g0, n), z_edge2], rly.at[pl.ds(g0, n)], l_s.at[cc], l_r.at[cc], dev(z_mid, q))

    @fenced
    def combine(cc):
        g0, n = CHUNKS[cc]
        rows_in = rbuf.at[pl.ds(g0, n)]
        rcopy(rows_in, rows_in, s_s.at[cc, 0], s_r.at[cc], dev(z, qc)).wait_recv()
        got = jnp.concatenate([jnp.concatenate([sbuf[g0 + t, q]] + [rbuf[g0 + t, j] for j in range(3)], axis=0) for t in range(n)], axis=1)
        acc = dot(w3[0], got) + (dot(w3[1], got) + dot(w3[2], got))
        for t in range(n):
            fbuf[g0 + t] = acc[:, t * LANE:(t + 1) * LANE].reshape(SRC, rows, LANE)

        @pl.when(edge)
        def _():
            if cc in DIRECT:
                f_copy(cc, z_edge2, 2, 2).start()
            else:
                l_copy(cc).start()
            f_copy(cc, z_mid2, 1, 2).start()
            f_copy(cc, z_mid, 0, 0).start()

        @pl.when(jnp.logical_not(edge))
        def _():
            if cc in DIRECT:
                f_copy(cc, z_edge2, 2, 1).start()
            f_copy(cc, z_mid2, 1, 1).start()
            f_copy(cc, z_edge, 0, 0).start()

    @fenced
    def relay(cc):
        g0, n = CHUNKS[cc]

        @pl.when(jnp.logical_not(edge))
        def _():
            l_copy(cc).wait_recv()
            for t in range(g0, g0 + n):
                fbuf[t, z_edge2] += rly[t]
            f_copy(cc, z_edge2, 2, 1).start()

    @fenced
    def final(cc):
        g0, n = CHUNKS[cc]

        def finish(parts):
            sums = zbuf.at[pl.ds(g0, n), pl.ds(0, parts)]
            rcopy(sums, sums, f_s.at[cc, 0], f_r.at[cc], dev(z, qc)).wait_recv()
            for t in range(g0, g0 + n):
                cols = pl.ds(t * LANE, LANE)
                tot = fbuf[t, z]
                for rk in range(parts):
                    tot = tot + zbuf[t, rk]
                sh = sout[t * LANE // cw, :, pl.ds(t * LANE % cw, LANE)]
                out_ref[:, cols] = (res_ref[:, cols].astype(f32) + sh + tot).astype(bf16)

        @pl.when(edge)
        def _():
            finish(3 if cc in DIRECT else 2)

        @pl.when(jnp.logical_not(edge))
        def _():
            finish(3)

    @fenced
    def drain_gather():
        for p in range(NP // 2, NP):
            @pl.when(z < 3)
            def _():
                xup(p).wait_send()

            @pl.when(z > 0)
            def _():
                xdn(p).wait_send()

            @pl.when((z == 0) | (z == 3))
            def _():
                ysend(blk(q, z, p), z, p).wait_send()
        for p in range(NP):
            for b in range(SRC):
                if p < NP // 2 or b in (1, 2):
                    ysend(blk(q, b, p), b, p).wait_send()
        for b in range(SRC):
            whole = hall.at[q, b]

            @pl.when((z < 3) & (b <= z))
            def _():
                rcopy(whole, whole, zup_s.at[b], z_r.at[b, 0], dev(z + 1, q)).wait_send()

            @pl.when((z > 0) & (b >= z))
            def _():
                rcopy(whole, whole, zdn_s.at[b], z_r.at[b, 0], dev(z - 1, q)).wait_send()
            for k in range(2):
                rcopy(whole, whole, c_s.at[k, b], c_r.at[k, 0], dev(z, qc)).wait_send()

    @fenced
    def drain(cc):
        for j in range(3):
            s_copy(cc, j).wait_send()
        f_copy(cc, z_mid, 0, 0).wait_send()
        f_copy(cc, z_mid, 1, 0).wait_send()
        if cc in DIRECT:
            f_copy(cc, z_mid, 2, 0).wait_send()
            return

        @pl.when(edge)
        def _():
            l_copy(cc).wait_send()

        @pl.when(jnp.logical_not(edge))
        def _():
            f_copy(cc, z_edge2, 2, 1).wait_send()

    for cc in range(AHEAD):
        down(cc)
    spread()
    for cc in range(last + 1):
        if cc + AHEAD <= last:
            down(cc + AHEAD)
        if cc == AHEAD:
            drain_gather()
        if cc >= SETTLED:
            drain(cc - SETTLED)
        combine(cc)
        if cc and cc - 1 not in DIRECT:
            relay(cc - 1)
    for cc in range(last + 1):
        final(cc)
    for cc in range(last + 1 - SETTLED, last + 1):
        drain(cc)


def moe_call(hx, resid, router, sh_gate, sh_up, sh_down, ex_gate, ex_up, ex_down):
    rows, dm = resid.shape
    ff = ex_gate.shape[2]
    cw = dm // NCH
    bf16, f32 = jnp.bfloat16, jnp.float32
    vm = pl.BlockSpec(memory_space=pltpu.VMEM)
    hb = pl.BlockSpec(memory_space=pl.ANY)
    sem = pltpu.SemaphoreType.DMA
    nk = NE * GRP
    return pl.pallas_call(
        moe_kernel,
        out_shape=jax.ShapeDtypeStruct((rows, dm), bf16),
        in_specs=[vm] * 3 + [hb] * 6,
        out_specs=vm,
        scratch_shapes=[
            pltpu.VMEM((4, SRC, rows, dm + LANE), bf16),
            pltpu.VMEM((NE, 4, GRP, dm), bf16),
            pltpu.VMEM((NE, SRC * GRP, ff), bf16),
            pltpu.VMEM((2, rows, ff), bf16),
            pltpu.VMEM((NCH, rows, cw), f32),
            pltpu.VMEM((NA, dm, ff), bf16),
            pltpu.VMEM((NB, NE, ff, cw), bf16),
            pltpu.VMEM((dm // LANE, 4, nk, LANE), bf16),
            pltpu.VMEM((dm // LANE, 3, nk, LANE), bf16),
            pltpu.VMEM((dm // LANE, SRC, rows, LANE), f32),
            pltpu.VMEM((dm // LANE, 3, rows, LANE), f32),
            pltpu.VMEM((dm // LANE, rows, LANE), f32),
            pltpu.VMEM((3, SRC * rows, SRC * nk), bf16),
            pltpu.VMEM((4, nk, SRC * rows), bf16),
            sem((NA,)), sem((NB, 2)),
            sem((4,)), sem((4,)), sem((4, NP)),
            sem((4, NP)), sem((4, NP)),
            sem((NP,)), sem((NP,)), sem((2, NP)),
            sem((2, 4)), sem((2, NP)),
            sem((len(CHUNKS), 3)), sem((len(CHUNKS),)),
            sem((len(CHUNKS), 3)), sem((len(CHUNKS),)),
            sem((len(CHUNKS),)), sem((len(CHUNKS),)),
        ],
        compiler_params=pltpu.CompilerParams(collective_id=0, has_side_effects=True, vmem_limit_bytes=66 * 1024 * 1024 - 2 * 1024 * 1024 - 65536),
        name="moe",
    )(hx, resid, router.T, sh_gate, sh_up, sh_down.reshape(2, ff, dm), ex_gate, ex_up, ex_down)


def solution(mesh):
    row_one = P(('dp', 'ep'))
    row_two = P(('dp', 'ep'), None)
    row_three = P(('dp', 'ep'), None, None)
    rep_one = P(None)
    rep_two = P(None, None)
    rep_three = P(None, None, None)
    exp_spec = P('ep', None, None)

    def local_step(tok_in, lat_cache, rope_cache, tok_pos, expert_ids, attn_gain, w_query, w_kvdown, w_ukey, w_uval, w_out, ffn_gain, w_router, sh_gate, sh_up, sh_down, ex_gate, ex_up, ex_down):
        hx, resid, lat_out, rope_out = attn_call(tok_in, lat_cache, rope_cache, tok_pos, expert_ids, attn_gain, w_query, w_kvdown, w_ukey, w_uval, w_out, ffn_gain)
        out_hidden = moe_call(hx, resid, w_router, sh_gate, sh_up, sh_down, ex_gate, ex_up, ex_down)
        return out_hidden, lat_out, rope_out

    in_specs = (row_two, row_three, row_three, row_one, row_two, rep_one, rep_two, rep_two, rep_three, rep_three, rep_two, rep_one, rep_two, rep_two, rep_two, rep_two, exp_spec, exp_spec, exp_spec)
    out_specs = (row_two, row_three, row_three)
    return jax.shard_map(local_step, mesh=mesh, in_specs=in_specs, out_specs=out_specs, check_vma=False)
```
